256 devices in a mesh: pipe: 2 (over core), dp: 64 (over z, y, x_lo), tensor: 2 (over x_hi).
Axes of the slice: x: 4 (x_hi: 2, x_lo: 2; x = x_hi * 2 + x_lo), y: 4, z: 8, core: 2. Of those that a mesh axis runs over, the one named last changes fastest.
Arguments:
- hidden_in: bfloat16 [2, 128, 2, 64, 3584], P('pipe', 'dp'), may hold values from -60 to 60, as said below
- attention_probs: bfloat16 [2, 128, 2, 14, 64, 64], P('pipe', 'dp', None, 'tensor'), may hold values from 0 to 1, as said below
- norm_gain: float32 [2, 3584], P('pipe'), may hold values from 0.5 to 1.5
- value_weight: bfloat16 [2, 3584, 256], P('pipe', None, 'tensor'), may hold values from -0.09375 to 0.09375
- output_weight: bfloat16 [2, 1792, 3584], P('pipe', 'tensor'), may hold values from -0.125 to 0.125
- head_grad: bfloat16 [128, 2, 64, 3584], P('dp', 'tensor'), may hold values from -16 to 16
- policy_logprob: float32 [128, 2, 64], P('dp'), may hold values from -3 to -0.2
- reference_logprob: float32 [128, 2], P('dp'), may hold values from -96 to -12.8
- sequence_bounds: int32 [128, 3], P('dp'), may hold values from 1 to 64, as said below
Outputs:
- section_cotangent: bfloat16 [2, 128, 2, 64, 3584], P('pipe', 'dp', 'tensor')
- value_gradient: float32 [2, 3584, 256], P('pipe', 'dp', 'tensor')
- output_gradient: float32 [2, 3584, 1792], P('pipe', 'dp', 'tensor')
- gain_gradient: float32 [2, 3584], P('pipe', 'dp')
The draws below stay inside these ranges and needn't reach their ends.
Inputs may be any that keep to these rules, and one draw needn't show every extreme that they name: `sequence_bounds`: entry 0 is the prompt length, shared by the two sequences of a pair; a sequence's response is the positions from entry 0 up to its end (entry 1 for the chosen, entry 2 for the rejected sequence), and holds one position or more. `attention_probs`: each row is a causal attention distribution: zero above the diagonal, summing to one before rounding. `hidden_in`: activations of varying size from token to token.
All inputs are finite; a program needn't handle non-finite values.
Results may differ from the reference program's by a relative error of at most 0.017.
Values may be sent and summed in bfloat16 or wider, within the bound.
A program may use at most 128 MiB of HBM per device.

```python
import math
import jax
import jax.numpy as jnp
from jax import lax

D = 3584
HEADS = 14
KV_HEADS = 2
HEAD_DIM = 128
SEQ = 64
PAIRS = 128
N_PIPE = 2
N_TENSOR = 2


def draw_hidden_in(key, part):
    key_main, key_scale = jax.random.split(key, 2)
    full_shape = (N_PIPE, PAIRS, 2, SEQ, D)
    row_scale = jnp.exp(jax.random.uniform(key_scale, (N_PIPE, PAIRS, 2, SEQ, 1), jnp.float32, 0.0, math.log(10.0)))
    noise = jnp.clip(jax.random.normal(key_main, full_shape, jnp.float32), -6.0, 6.0)
    return (row_scale * noise).astype(jnp.bfloat16)


def draw_attention_probs(key, part):
    key_noise, key_temper, key_slope = jax.random.split(key, 3)
    full_shape = (N_PIPE, PAIRS, 2, HEADS, SEQ, SEQ)
    head_shape = (N_PIPE, 1, 1, HEADS, 1, 1)
    temper = jnp.exp(jax.random.uniform(key_temper, head_shape, jnp.float32, math.log(0.5), math.log(3.0)))
    decay_slope = jnp.exp(jax.random.uniform(key_slope, head_shape, jnp.float32, math.log(0.5 / SEQ), 0.0))
    query_pos = jnp.arange(SEQ)[:, None]
    key_pos = jnp.arange(SEQ)[None, :]
    distance = (query_pos - key_pos).astype(jnp.float32)
    logits = jax.random.normal(key_noise, full_shape, jnp.float32) * temper - decay_slope * distance
    logits = jnp.where(key_pos <= query_pos, logits, -1000000000.0)
    return jax.nn.softmax(logits, axis=-1).astype(jnp.bfloat16)


def draw_sequence_bounds(key, part):
    key_prompt, key_extra, key_pick = jax.random.split(key, 3)
    pair_index = jnp.arange(PAIRS, dtype=jnp.int32)
    prompt = jax.random.randint(key_prompt, (PAIRS,), 1, SEQ // 4 + 1, jnp.int32)
    base_length = SEQ // 8 + SEQ // 2 * pair_index // PAIRS
    extra = jax.random.randint(key_extra, (PAIRS, 2), 0, SEQ // 8 + 1, jnp.int32)
    ends = jnp.minimum(prompt[:, None] + base_length[:, None] + extra, SEQ)
    picked = jax.random.randint(key_pick, (), 0, PAIRS, jnp.int32)
    full_end = (pair_index == picked)[:, None] & (jnp.arange(2, dtype=jnp.int32)[None, :] == 1)
    ends = jnp.where(full_end, SEQ, ends)
    return jnp.concatenate([prompt[:, None], ends], axis=1).astype(jnp.int32)


def levels(stream_key, dims, shards, smallest, largest):
    def one(position, shards_of):
        steps = jax.random.uniform(jax.random.fold_in(jax.random.fold_in(stream_key, 6), position), (shards_of,), jnp.float32, smallest / len(shards), largest / len(shards))
        return jnp.repeat(jnp.exp(steps), dims[position] // shards_of).reshape((-1,) + (1,) * (len(dims) - position - 1))

    factor_of = one(*shards[0])
    for cut in shards[1:]:
        factor_of = factor_of * one(*cut)
    return factor_of


def gaussian(stream_key, dims, deviation, most, cuts=(), held_as=jnp.bfloat16):
    factor_of = levels(stream_key, dims, cuts, -0.22, 0.18) if cuts else 1.0
    drawn = jax.random.normal(stream_key, dims, jnp.float32) * deviation * factor_of
    return jnp.minimum(jnp.maximum(drawn, -most), most).astype(held_as)


def setup_inputs(seed: int = 0) -> dict:
    key_of = jax.random.split(jax.random.key(seed), 10)
    hidden_in = draw_hidden_in(jax.random.fold_in(key_of[9], 71), 0)
    attention_probs = draw_attention_probs(jax.random.fold_in(key_of[9], 71), 0)
    norm_gain = jnp.clip(1.0 + 0.1 * jax.random.normal(key_of[2], (N_PIPE, D), jnp.float32), 0.5, 1.5)
    value_weight = gaussian(key_of[3], (N_PIPE, D, KV_HEADS * HEAD_DIM), D ** -0.5, 0.09375, ((0, 2), (2, 2)))
    output_weight = gaussian(key_of[4], (N_PIPE, HEADS * HEAD_DIM, D), (HEADS * HEAD_DIM) ** -0.5, 0.125, ((0, 2), (1, 2)))
    head_grad = gaussian(key_of[5], (PAIRS, 2, SEQ, D), 4.0, 16.0, ((0, 64), (1, 2)))
    policy_logprob = jnp.clip(-3.0 + 2.8 * jax.random.uniform(key_of[6], (PAIRS, 2, SEQ), jnp.float32) ** levels(key_of[6], (PAIRS, 2, SEQ), ((0, 64),), -0.2, 0.2), -3.0, -0.2)
    reference_logprob = jnp.clip(-96.0 + 83.2 * jax.random.uniform(key_of[7], (PAIRS, 2), jnp.float32) ** levels(key_of[7], (PAIRS, 2), ((0, 64),), -0.2, 0.2), -96.0, -12.8)
    sequence_bounds = draw_sequence_bounds(jax.random.fold_in(key_of[9], 71), 0)
    return dict(hidden_in=hidden_in, attention_probs=attention_probs, norm_gain=norm_gain, value_weight=value_weight, output_weight=output_weight, head_grad=head_grad, policy_logprob=policy_logprob, reference_logprob=reference_logprob, sequence_bounds=sequence_bounds)


EPSILON = 1e-06
DPO_BETA = 0.25
LIKELIHOOD_COEF = 0.2

def section_backward(inputs, pattern, gain_vector, value_matrix, output_matrix, upstream):
    group_size = HEADS // KV_HEADS
    input_float = inputs.astype(jnp.float32)
    inverse_rms = lax.rsqrt(lax.optimization_barrier(jnp.mean(input_float * input_float, axis=-1, keepdims=True)) + EPSILON)
    normed = (input_float * inverse_rms * gain_vector).astype(jnp.bfloat16)
    values = jnp.einsum('pcsd,dk->pcsk', normed.astype(jnp.float32), value_matrix.astype(jnp.float32)).astype(jnp.bfloat16)
    grouped = pattern.astype(jnp.float32).reshape(PAIRS, 2, KV_HEADS, group_size, SEQ, SEQ)
    values_heads = values.astype(jnp.float32).reshape(PAIRS, 2, SEQ, KV_HEADS, HEAD_DIM)
    mixed = jnp.einsum('pckgst,pctke->pcskge', grouped, values_heads).astype(jnp.bfloat16)
    mixed = mixed.reshape(PAIRS, 2, SEQ, HEADS * HEAD_DIM)
    upstream_float = upstream.astype(jnp.float32)
    mixed_grad = jnp.einsum('pcsd,hd->pcsh', upstream_float, output_matrix.astype(jnp.float32)).astype(jnp.bfloat16)
    mixed_heads = mixed_grad.astype(jnp.float32).reshape(PAIRS, 2, SEQ, KV_HEADS, group_size, HEAD_DIM)
    values_grad = jnp.einsum('pckgst,pcskge->pctke', grouped, mixed_heads).astype(jnp.bfloat16)
    values_grad = values_grad.reshape(PAIRS, 2, SEQ, KV_HEADS * HEAD_DIM)
    group_columns = KV_HEADS * HEAD_DIM // N_TENSOR
    grad_groups = values_grad.astype(jnp.float32).reshape(PAIRS, 2, SEQ, N_TENSOR, group_columns)
    weight_groups = value_matrix.astype(jnp.float32).reshape(D, N_TENSOR, group_columns)
    normed_grad = jnp.zeros((PAIRS, 2, SEQ, D), jnp.float32)
    for group_index in range(N_TENSOR):
        group_term = jnp.einsum('pcsk,dk->pcsd', grad_groups[:, :, :, group_index, :], weight_groups[:, group_index, :])
        rounded = lax.optimization_barrier(group_term.astype(jnp.bfloat16))
        normed_grad = normed_grad + rounded.astype(jnp.float32)
    gain_total = lax.optimization_barrier(jnp.sum(normed_grad * input_float * inverse_rms, axis=(0, 1, 2)))
    scaled = normed_grad * gain_vector
    cubed = inverse_rms * inverse_rms * inverse_rms
    input_grad = inverse_rms * scaled - input_float * cubed * lax.optimization_barrier(jnp.mean(input_float * scaled, axis=-1, keepdims=True))
    new_rows = (upstream_float + input_grad).astype(jnp.bfloat16)
    mixed_total = jnp.einsum('pcsd,pcsh->dh', upstream_float, mixed.astype(jnp.float32))
    value_total = jnp.einsum('pcsd,pcsk->dk', normed.astype(jnp.float32), values_grad.astype(jnp.float32))
    return (new_rows, value_total, mixed_total, gain_total)

def reference(hidden_in, attention_probs, norm_gain, value_weight, output_weight, head_grad, policy_logprob, reference_logprob, sequence_bounds):
    positions = jnp.arange(SEQ, dtype=jnp.int32)
    response_bool = (positions[None, None, :] >= sequence_bounds[:, 0:1, None]) & (positions[None, None, :] < sequence_bounds[:, 1:3, None])
    response_mask = response_bool.astype(jnp.float32)
    sequence_logprob = lax.optimization_barrier(jnp.sum(response_mask * policy_logprob, axis=-1))
    margin = DPO_BETA * (sequence_logprob[:, 0] - reference_logprob[:, 0] - (sequence_logprob[:, 1] - reference_logprob[:, 1]))
    weight_pair = jax.nn.sigmoid(-margin)
    chosen_total = jnp.sum(response_bool[:, 0, :].astype(jnp.int32))
    likelihood_scale = LIKELIHOOD_COEF * jnp.asarray(PAIRS, jnp.float32) / chosen_total.astype(jnp.float32)
    chosen_weight = -DPO_BETA * weight_pair[:, None] * response_mask[:, 0] - likelihood_scale * response_mask[:, 0]
    rejected_weight = DPO_BETA * weight_pair[:, None] * response_mask[:, 1]
    token_weight = jnp.stack([chosen_weight, rejected_weight], axis=1)
    upstream = (token_weight[..., None] * head_grad.astype(jnp.float32)).astype(jnp.bfloat16)
    cotangents = []
    value_list = []
    output_list = []
    gain_list = []
    for section_index in range(N_PIPE - 1, -1, -1):
        upstream, value_total, mixed_total, gain_total = section_backward(hidden_in[section_index], attention_probs[section_index], norm_gain[section_index], value_weight[section_index], output_weight[section_index], upstream)
        cotangents.insert(0, upstream)
        value_list.insert(0, value_total)
        output_list.insert(0, mixed_total)
        gain_list.insert(0, gain_total)
    return (jnp.stack(cotangents), jnp.stack(value_list), jnp.stack(output_list), jnp.stack(gain_list))
```

```python
import functools

import jax
import jax.numpy as jnp
from jax import lax
from jax.experimental import pallas as pl
from jax.experimental.pallas import tpu as pltpu
from jax.sharding import PartitionSpec as P

HEAD_DIM = 128
EPSILON = 1e-06
DPO_BETA = 0.25
LIKELIHOOD_COEF = 0.2
MESH = pl.DeviceIdType.MESH
BF = jnp.bfloat16
F32 = jnp.float32
COLS = 512


class Flow:
    def __init__(self, size, place, ahead, behind, local, landing, sends, receives, base, hops):
        self.size, self.place = size, place
        self.target = {1: ahead, -1: behind}
        self.local, self.landing = local, landing
        self.sends, self.receives = sends, receives
        self.hops = hops
        self.slot = {}
        for (way, half), count in hops.items():
            for step in range(count):
                self.slot[way, half, step] = base + len(self.slot)
        self.count = len(self.slot)
        self.copies = {}

    def copy(self, way, half, step):
        slot = self.slot[way, half, step]
        chunk = lax.rem(self.place + way * (self.hops[way, half] - step) + self.size, self.size)
        return chunk, pltpu.make_async_remote_copy(
            src_ref=self.local(chunk, half),
            dst_ref=self.landing(slot),
            send_sem=self.sends.at[slot],
            recv_sem=self.receives.at[slot],
            device_id=self.target[way],
            device_id_type=MESH,
        )

    def collect(self, way, half, step, chunk):
        self.copies[way, half, step].wait_recv()
        target = self.local(chunk, half)
        landed = self.landing(self.slot[way, half, step])
        add_into(target, landed)

    def step(self, step):
        for way, half in self.hops:
            if step < self.hops[way, half]:
                chunk, copy = self.copy(way, half, step)
                if step:
                    self.collect(way, half, step - 1, chunk)
                copy.start()
                self.copies[way, half, step] = copy

    def finish(self):
        for (way, half), count in self.hops.items():
            self.collect(way, half, count - 1, self.place)

    def drain(self):
        for copy in self.copies.values():
            copy.wait_send()


def add_into(target, landed):
    if len(target.shape) > 2 and target.shape[-2] > 1:

        def one(index, carry):
            target[index] = target[index] + landed[index]
            return carry

        lax.fori_loop(0, target.shape[0], one, 0)
    else:
        target[...] = target[...] + landed[...]


def scatter_kernel(
    mixed_hbm,
    value_hbm,
    gain_hbm,
    mixed_out,
    value_out,
    gain_out,
    part_a,
    part_b,
    part_g,
    land_a1,
    land_b1,
    land_a2,
    land_b2,
    land_g1,
    land_g2,
    last_src,
    last_dst,
    last_g,
    load_sems,
    sends,
    receives,
):
    pipe = lax.axis_index("pipe")
    tensor = lax.axis_index("tensor")
    dp = lax.axis_index("dp")
    z = dp // 8
    y = lax.rem(dp, 8) // 2
    x = lax.rem(dp, 2)

    def device(z_at, y_at, x_at):
        return (pipe, z_at * 8 + y_at * 2 + x_at, tensor)

    z_next, z_prev = lax.rem(z + 1, 8), lax.rem(z + 7, 8)
    y_next, y_prev = lax.rem(y + 1, 4), lax.rem(y + 3, 4)
    z_ways = (device(z_next, y, x), device(z_prev, y, x))
    y_ways = (device(z, y_next, x), device(z, y_prev, x))
    x_way = device(z, y, 1 - x)
    loads = [
        pltpu.make_async_copy(mixed_hbm.at[:, :, :, pl.ds(0, COLS)], part_a, load_sems.at[0]),
        pltpu.make_async_copy(
            mixed_hbm.at[:, :, :, pl.ds(COLS, COLS - HEAD_DIM)],
            part_b.at[:, :, :, pl.ds(0, COLS - HEAD_DIM)],
            load_sems.at[1],
        ),
        pltpu.make_async_copy(
            value_hbm, part_b.at[:, :, :, pl.ds(COLS - HEAD_DIM, HEAD_DIM)], load_sems.at[2]
        ),
        pltpu.make_async_copy(gain_hbm, part_g, load_sems.at[3]),
    ]
    for load in loads:
        load.start()
    barrier = pltpu.get_barrier_semaphore()
    for neighbour in (*z_ways, *y_ways, x_way):
        pl.semaphore_signal(barrier, inc=1, device_id=neighbour, device_id_type=MESH)
    pl.semaphore_wait(barrier, 5)
    for load in loads:
        load.wait()

    base = 0

    def flow(size, place, ways, local, landing, hops):
        nonlocal base
        first = base
        made = Flow(
            size, place, *ways, local, lambda slot: landing.at[slot - first], sends, receives, base, hops
        )
        base += made.count
        return made

    z_halves = {(1, 0): 4, (-1, 1): 4, (1, 1): 3, (-1, 0): 3}
    y_halves = {(1, 0): 2, (-1, 1): 2, (1, 1): 1, (-1, 0): 1}
    z_whole = {(1, 0): 4, (-1, 0): 3}
    y_whole = {(1, 0): 2, (-1, 0): 1}
    a1 = flow(8, z, z_ways, lambda q, h: part_a.at[q, pl.ds(2 * h, 2)], land_a1, z_halves)
    b1 = flow(4, y, y_ways, lambda q, h: part_b.at[pl.ds(4 * h, 4), q], land_b1, y_halves)
    a2 = flow(4, y, y_ways, lambda q, h: part_a.at[z, q], land_a2, y_whole)
    b2 = flow(8, z, z_ways, lambda q, h: part_b.at[q, y], land_b2, z_whole)
    g1 = flow(8, z, z_ways, lambda q, h: part_g.at[q], land_g1, z_whole)
    g2 = flow(4, y, y_ways, lambda q, h: part_g.at[z, q], land_g2, y_whole)

    def last(index, source, target):
        return pltpu.make_async_remote_copy(
            src_ref=source,
            dst_ref=target,
            send_sem=sends.at[base + index],
            recv_sem=receives.at[base + index],
            device_id=x_way,
            device_id_type=MESH,
        )

    def exchange(index, part):
        total = part[z, y].astype(F32)
        low, high = total[:56], total[56:]
        last_src[index] = jnp.where(x == 0, high, low).astype(BF)
        copy = last(index, last_src.at[index], last_dst.at[index])
        copy.start()
        return copy, jnp.where(x == 0, low, high)

    a1.step(0)
    b1.step(0)
    g1.step(0)
    a1.step(1)
    b1.step(1)
    g1.step(1)
    a1.step(2)
    g1.step(2)
    a1.step(3)
    g1.step(3)
    b1.finish()
    b2.step(0)
    a1.finish()
    a2.step(0)
    g1.finish()
    g2.step(0)
    b2.step(1)
    a2.step(1)
    g2.step(1)
    b2.step(2)
    a2.finish()
    copy_a, own_a = exchange(0, part_a)
    mixed_out[:, :COLS] = own_a
    g2.finish()
    copy_g = last(2, part_g.at[z, y], last_g)
    copy_g.start()
    b2.step(3)
    b2.finish()
    copy_b, own_b = exchange(1, part_b)
    mixed_out[:, COLS:] = own_b[:, : COLS - HEAD_DIM]
    value_out[...] = own_b[:, COLS - HEAD_DIM :]
    copy_a.wait_recv()
    mixed_out[:, :COLS] += last_dst[0].astype(F32)
    copy_g.wait_recv()
    gain_out[...] = part_g[z, y] + last_g[...]
    copy_b.wait_recv()
    landed = last_dst[1].astype(F32)
    mixed_out[:, COLS:] += landed[:, : COLS - HEAD_DIM]
    value_out[...] += landed[:, COLS - HEAD_DIM :]
    for made in (a1, b1, a2, b2, g1, g2):
        made.drain()
    for copy in (copy_a, copy_b, copy_g):
        copy.wait_send()


def reduce_scatter(mixed_part, value_part, gain_part):
    width = mixed_part.shape[1]
    copies = 14 + 6 + 3 + 7 + 7 + 3 + 3
    vmem = pl.BlockSpec(memory_space=pltpu.VMEM)
    hbm = pl.BlockSpec(memory_space=pl.ANY)
    gain_rows = jnp.pad(gain_part.reshape(8, 4, 1, 112), ((0, 0), (0, 0), (0, 0), (0, 16)))
    return pl.pallas_call(
        scatter_kernel,
        out_shape=(
            jax.ShapeDtypeStruct((56, width), F32),
            jax.ShapeDtypeStruct((56, HEAD_DIM), F32),
            jax.ShapeDtypeStruct((1, 128), F32),
        ),
        in_specs=[hbm, hbm, hbm],
        out_specs=(vmem, vmem, vmem),
        scratch_shapes=[
            pltpu.VMEM((8, 4, 112, COLS), BF),
            pltpu.VMEM((8, 4, 112, COLS), BF),
            pltpu.VMEM((8, 4, 1, 128), F32),
            pltpu.VMEM((14, 2, 112, COLS), BF),
            pltpu.VMEM((6, 4, 112, COLS), BF),
            pltpu.VMEM((3, 112, COLS), BF),
            pltpu.VMEM((7, 112, COLS), BF),
            pltpu.VMEM((7, 4, 1, 128), F32),
            pltpu.VMEM((3, 1, 128), F32),
            pltpu.VMEM((2, 56, COLS), BF),
            pltpu.VMEM((2, 56, COLS), BF),
            pltpu.VMEM((1, 128), F32),
            pltpu.SemaphoreType.DMA((4,)),
            pltpu.SemaphoreType.DMA((copies,)),
            pltpu.SemaphoreType.DMA((copies,)),
        ],
        compiler_params=pltpu.CompilerParams(
            collective_id=0, has_side_effects=True, vmem_limit_bytes=40 * 1024 * 1024
        ),
    )(
        mixed_part.reshape(8, 4, 112, width),
        value_part.reshape(8, 4, 112, HEAD_DIM),
        gain_rows,
    )


def body(
    hidden_in,
    attention_probs,
    norm_gain,
    value_weight,
    output_weight,
    head_grad,
    policy_logprob,
    reference_logprob,
    sequence_bounds,
):
    section = lax.axis_index("pipe")
    tensor_index = lax.axis_index("tensor")
    pairs, _, length, width = hidden_in.shape[1:]
    tokens = pairs * 2 * length
    heads = attention_probs.shape[3]
    gain_vector = norm_gain[0]
    value_matrix = value_weight[0]
    output_matrix = output_weight[0]
    pattern = attention_probs[0].reshape(pairs * 2, heads, length, length)
    inputs = hidden_in[0].reshape(tokens, width)

    other_head = lax.ppermute(head_grad, ("pipe", "tensor"), [(2, 3), (3, 2)])
    other_matrix = lax.ppermute(value_matrix, "tensor", [(0, 1), (1, 0)])

    positions = jnp.arange(length, dtype=jnp.int32)
    response_bool = (positions[None, None, :] >= sequence_bounds[:, 0:1, None]) & (
        positions[None, None, :] < sequence_bounds[:, 1:3, None]
    )
    response_mask = response_bool.astype(F32)
    sequence_logprob = jnp.sum(response_mask * policy_logprob, axis=-1)
    margin = DPO_BETA * (
        sequence_logprob[:, 0]
        - reference_logprob[:, 0]
        - (sequence_logprob[:, 1] - reference_logprob[:, 1])
    )
    weight_pair = jax.nn.sigmoid(-margin)
    local_count = jnp.sum(response_bool[:, 0, :].astype(jnp.int32))
    chosen_total = lax.psum(local_count, "dp")
    pair_total = pairs * lax.axis_size("dp")
    likelihood_scale = (
        LIKELIHOOD_COEF * jnp.asarray(pair_total, F32) / chosen_total.astype(F32)
    )
    chosen_weight = (
        -DPO_BETA * weight_pair[:, None] * response_mask[:, 0]
        - likelihood_scale * response_mask[:, 0]
    )
    rejected_weight = DPO_BETA * weight_pair[:, None] * response_mask[:, 1]
    token_weight = jnp.stack([chosen_weight, rejected_weight], axis=1)

    input_float = inputs.astype(F32)
    inverse_rms = lax.rsqrt(jnp.mean(input_float * input_float, axis=-1, keepdims=True) + EPSILON)
    normed = (input_float * inverse_rms * gain_vector).astype(BF)
    values = jnp.dot(normed, value_matrix, preferred_element_type=F32).astype(BF)
    values = values.reshape(pairs * 2, length, HEAD_DIM)
    mixed = jnp.einsum("nhqk,nke->nqhe", pattern, values, preferred_element_type=F32)
    mixed = mixed.astype(BF).reshape(tokens, heads * HEAD_DIM)

    def through(upstream):
        mixed_grad = jnp.einsum(
            "nd,hd->nh", upstream, output_matrix, preferred_element_type=F32
        ).astype(BF)
        mixed_heads = mixed_grad.reshape(pairs * 2, length, heads, HEAD_DIM)
        values_grad = jnp.einsum(
            "nhqk,nqhe->nke", pattern, mixed_heads, preferred_element_type=F32
        )
        values_grad = values_grad.astype(BF).reshape(tokens, HEAD_DIM)
        other_grad = lax.ppermute(values_grad, "tensor", [(0, 1), (1, 0)])
        normed_grad = jnp.einsum(
            "nk,dk->nd", values_grad, value_matrix, preferred_element_type=F32
        ).astype(BF).astype(F32) + jnp.einsum(
            "nk,dk->nd", other_grad, other_matrix, preferred_element_type=F32
        ).astype(BF).astype(F32)
        scaled = normed_grad * gain_vector
        cubed = inverse_rms * inverse_rms * inverse_rms
        input_grad = inverse_rms * scaled - input_float * cubed * jnp.mean(
            input_float * scaled, axis=-1, keepdims=True
        )
        below = (upstream.astype(F32) + input_grad).astype(BF)
        gain_terms = jnp.sum(normed_grad * input_float * inverse_rms, axis=0)
        return below, gain_terms, values_grad

    both = jnp.where(
        tensor_index == 0,
        jnp.concatenate([head_grad, other_head], axis=1),
        jnp.concatenate([other_head, head_grad], axis=1),
    )
    top = (token_weight[..., None] * both.astype(F32)).astype(BF).reshape(tokens, width)
    below_top, _, _ = through(top)
    passed = lax.ppermute(below_top, "pipe", [(1, 0)])
    upstream = jnp.where(section == 1, top, passed)
    below, gain_terms, values_grad = through(upstream)
    own_output = lax.dynamic_slice_in_dim(
        below.reshape(pairs, 2, length, width), tensor_index, 1, 1
    )
    value_part = jnp.einsum("nd,nk->dk", normed, values_grad, preferred_element_type=F32)
    mixed_part = jnp.einsum("nd,nh->dh", upstream, mixed, preferred_element_type=F32)
    mixed_share, value_share, gain_share = reduce_scatter(
        mixed_part.astype(BF), value_part.astype(BF), gain_terms
    )
    x = lax.rem(lax.axis_index("dp"), 2)
    gain_rows = lax.dynamic_slice_in_dim(gain_share[0], x * 56, 56, 0)
    return (own_output[None], value_share[None], mixed_share[None], gain_rows[None])


def solution(mesh):
    in_specs = (
        P("pipe", "dp", None, None, None),
        P("pipe", "dp", None, "tensor", None, None),
        P("pipe", None),
        P("pipe", None, "tensor"),
        P("pipe", "tensor", None),
        P("dp", "tensor", None, None),
        P("dp", None, None),
        P("dp", None),
        P("dp", None),
    )
    out_specs = (
        P("pipe", "dp", "tensor", None, None),
        P("pipe", "dp", "tensor"),
        P("pipe", "dp", "tensor"),
        P("pipe", "dp"),
    )
    return jax.shard_map(body, mesh=mesh, in_specs=in_specs, out_specs=out_specs, check_vma=False)
```

```python
import functools

import jax
import jax.numpy as jnp
from jax import lax
from jax.experimental import pallas as pl
from jax.experimental.pallas import tpu as pltpu
from jax.sharding import PartitionSpec as P

HEAD_DIM = 128
EPSILON = 1e-06
DPO_BETA = 0.25
LIKELIHOOD_COEF = 0.2
MESH = pl.DeviceIdType.MESH
BF = jnp.bfloat16
F32 = jnp.float32
COLS = 512


class Flow:
    def __init__(self, size, place, ahead, behind, local, landing, sends, receives, base, hops):
        self.size, self.place = size, place
        self.target = {1: ahead, -1: behind}
        self.local, self.landing = local, landing
        self.sends, self.receives = sends, receives
        self.hops = hops
        self.slot = {}
        for (way, half), count in hops.items():
            for step in range(count):
                self.slot[way, half, step] = base + len(self.slot)
        self.count = len(self.slot)
        self.copies = {}

    def copy(self, way, half, step):
        slot = self.slot[way, half, step]
        chunk = lax.rem(self.place + way * (self.hops[way, half] - step) + self.size, self.size)
        return chunk, pltpu.make_async_remote_copy(
            src_ref=self.local(chunk, half),
            dst_ref=self.landing(slot),
            send_sem=self.sends.at[slot],
            recv_sem=self.receives.at[slot],
            device_id=self.target[way],
            device_id_type=MESH,
        )

    def collect(self, way, half, step, chunk):
        self.copies[way, half, step].wait_recv()
        target = self.local(chunk, half)
        landed = self.landing(self.slot[way, half, step])
        add_into(target, landed)

    def step(self, step):
        for way, half in self.hops:
            if step < self.hops[way, half]:
                chunk, copy = self.copy(way, half, step)
                if step:
                    self.collect(way, half, step - 1, chunk)
                copy.start()
                self.copies[way, half, step] = copy

    def finish(self):
        for (way, half), count in self.hops.items():
            self.collect(way, half, count - 1, self.place)

    def drain(self):
        for copy in self.copies.values():
            copy.wait_send()


def add_into(target, landed):
    if len(target.shape) > 2 and target.shape[-2] > 1:

        def one(index, carry):
            target[index] = target[index] + landed[index]
            return carry

        lax.fori_loop(0, target.shape[0], one, 0)
    else:
        target[...] = target[...] + landed[...]


class Spread:
    def __init__(self, size, place, ahead, behind, own, landing, sends, receives, base):
        self.own, self.landing = own, landing
        self.sends, self.receives = sends, receives
        self.target = {1: ahead, -1: behind}
        self.hops = {1: size // 2, -1: size - 1 - size // 2}
        self.base = base
        self.count = size - 1
        self.copies = {}

    def slot(self, way, step):
        return step if way == 1 else self.hops[1] + step

    def step(self, step):
        for way, count in self.hops.items():
            if step < count:
                if step:
                    self.copies[way, step - 1].wait_recv()
                slot = self.slot(way, step)
                source = self.landing.at[self.slot(way, step - 1)] if step else self.own
                copy = pltpu.make_async_remote_copy(
                    src_ref=source,
                    dst_ref=self.landing.at[slot],
                    send_sem=self.sends.at[self.base + slot],
                    recv_sem=self.receives.at[self.base + slot],
                    device_id=self.target[way],
                    device_id_type=MESH,
                )
                copy.start()
                self.copies[way, step] = copy

    def finish(self):
        for way, count in self.hops.items():
            if count:
                self.copies[way, count - 1].wait_recv()
        total = self.own[...]
        for slot in range(self.count):
            total = total + self.landing[slot]
        return total

    def drain(self):
        for copy in self.copies.values():
            copy.wait_send()


WIDTH = 3584
TOKENS = 256
BLOCK = 256
BLOCKS = WIDTH // BLOCK
LENGTH = 64
HEADS = 7


def wide(rows):
    return jnp.concatenate([rows, rows], axis=1)


def step_kernel(
    bounds,
    reference,
    logprob,
    gain,
    inputs_hbm,
    pattern_hbm,
    value_hbm,
    output_hbm,
    head_hbm,
    mixed_out,
    value_out,
    gain_out,
    cotangent_out,
    inputs,
    pattern,
    weight,
    weight_other,
    weight_out,
    head_own,
    head_other,
    upstream,
    below,
    normed,
    values,
    mixed,
    mixed_grad,
    grad,
    grad_other,
    normed_grad,
    rms,
    gain_row,
    counts,
    land_cz,
    land_cy,
    land_cx,
    part_a,
    part_b,
    part_g,
    land_a1,
    land_b1,
    land_a2,
    land_b2,
    land_g1,
    land_g2,
    last_src,
    last_dst,
    last_g,
    load_sems,
    pass_sends,
    pass_receives,
    go,
    sends,
    receives,
):
    pipe = lax.axis_index("pipe")
    tensor = lax.axis_index("tensor")
    dp = lax.axis_index("dp")
    z = dp // 8
    y = lax.rem(dp, 8) // 2
    x = lax.rem(dp, 2)

    def device(z_at, y_at, x_at):
        return (pipe, z_at * 8 + y_at * 2 + x_at, tensor)

    z_next, z_prev = lax.rem(z + 1, 8), lax.rem(z + 7, 8)
    y_next, y_prev = lax.rem(y + 1, 4), lax.rem(y + 3, 4)
    z_ways = (device(z_next, y, x), device(z_prev, y, x))
    y_ways = (device(z, y_next, x), device(z, y_prev, x))
    x_way = device(z, y, 1 - x)
    peer = (pipe, dp, 1 - tensor)
    cross = (pipe, z * 8 + y * 2 + 1 - x, 1 - tensor)
    partner = (1 - pipe, dp, tensor)

    loads = {
        name: pltpu.make_async_copy(source, target, load_sems.at[index])
        for index, (name, source, target) in enumerate(
            (
                ("inputs", inputs_hbm, inputs),
                ("weight", value_hbm, weight),
                ("pattern", pattern_hbm, pattern),
                ("head", head_hbm, head_own),
                ("output", output_hbm, weight_out),
            )
        )
    }
    for load in loads.values():
        load.start()

    def token_rows(pair, which):
        lanes = lax.broadcasted_iota(jnp.int32, (1, LENGTH), 1)
        rows = lax.broadcasted_iota(jnp.int32, (LENGTH, 1), 0)
        first, end = bounds[pair, 0], bounds[pair, 1 + which]
        row_mask = ((lanes >= first) & (lanes < end)).astype(F32)
        column_mask = ((rows >= first) & (rows < end)).astype(F32)
        return row_mask, column_mask

    own_count = jnp.zeros((1, 1), F32)
    for pair in range(2):
        own_count = own_count + jnp.sum(token_rows(pair, 0)[0], axis=1, keepdims=True)
    counts[0] = jnp.broadcast_to(own_count, (1, 128))
    part_g[...] = jnp.zeros_like(part_g)

    barrier = pltpu.get_barrier_semaphore()
    for neighbour in (*z_ways, *y_ways, x_way, peer, cross, partner):
        pl.semaphore_signal(barrier, inc=1, device_id=neighbour, device_id_type=MESH)
    pl.semaphore_wait(barrier, 8)

    def passing(index, source, target, to):
        return pltpu.make_async_remote_copy(
            src_ref=source,
            dst_ref=target,
            send_sem=pass_sends.at[index],
            recv_sem=pass_receives.at[index],
            device_id=to,
            device_id_type=MESH,
        )

    send_head = passing(0, head_hbm, head_other, peer)
    send_weight = passing(1, value_hbm, weight_other, cross)
    send_grad = passing(2, grad, grad_other, peer)
    send_below = [
        passing(3 + pair, below.at[pl.ds(128 * pair, 128)], upstream.at[pl.ds(128 * pair, 128)], partner)
        for pair in range(2)
    ]

    @pl.when(pipe == 1)
    def _():
        send_head.start()

    base = 0

    def spread(size, place, ways, own, landing):
        nonlocal base
        made = Spread(size, place, *ways, own, landing, sends, receives, base)
        base += made.count
        return made

    count_z = spread(8, z, z_ways, counts.at[0], land_cz)
    count_y = spread(4, y, y_ways, counts.at[1], land_cy)
    count_x = spread(2, x, (x_way, x_way), counts.at[2], land_cx)

    count_z.step(0)
    loads["inputs"].wait()

    def square(index, total):
        at = pl.ds(pl.multiple_of(index * BLOCK, BLOCK), BLOCK)
        block = inputs[:, at].astype(F32)
        block = block * block
        return total + block[:, :128] + block[:, 128:]

    total = lax.fori_loop(0, BLOCKS, square, jnp.zeros((TOKENS, 128), F32))
    mean = jnp.sum(total, axis=1, keepdims=True) / WIDTH
    rms[...] = jnp.broadcast_to(lax.rsqrt(mean + EPSILON), (TOKENS, 128))
    count_z.step(1)
    loads["weight"].wait()

    def project(index, total):
        at = pl.ds(pl.multiple_of(index * BLOCK, BLOCK), BLOCK)
        block = (inputs[:, at].astype(F32) * wide(rms[...]) * gain[:, at]).astype(BF)
        normed[:, at] = block
        return total + jnp.dot(block, weight[at, :], preferred_element_type=F32)

    total = lax.fori_loop(0, BLOCKS // 2, project, jnp.zeros((TOKENS, 128), F32))
    count_z.step(2)
    total = lax.fori_loop(BLOCKS // 2, BLOCKS, project, total)
    values[...] = total.astype(BF)
    count_z.step(3)
    loads["pattern"].wait()

    def mix(index, carry):
        rows = pl.ds(pl.multiple_of(index * LENGTH, LENGTH), LENGTH)
        block = jnp.dot(pattern[index], values[rows, :], preferred_element_type=F32).astype(BF)
        for head in range(HEADS):
            mixed[rows, head * 128 : (head + 1) * 128] = block[head * LENGTH : (head + 1) * LENGTH]
        return carry

    lax.fori_loop(0, 2, mix, 0)
    counts[1] = count_z.finish()
    lax.fori_loop(2, 4, mix, 0)
    count_y.step(0)
    count_y.step(1)
    counts[2] = count_y.finish()
    loads["head"].wait()
    count_x.step(0)
    total_count = count_x.finish()[:, :1]
    loads["output"].wait()

    @pl.when(pipe == 1)
    def _():
        scale = jnp.full((1, 1), LIKELIHOOD_COEF * 128, F32) / total_count
        for pair in range(2):
            masks = [token_rows(pair, which) for which in range(2)]
            sums = [
                jnp.sum(masks[which][0] * logprob[pair, which : which + 1, :], axis=1, keepdims=True)
                for which in range(2)
            ]
            margin = DPO_BETA * (
                sums[0] - reference[pair, 0] - (sums[1] - reference[pair, 1])
            )
            pair_weight = jax.nn.sigmoid(-margin)
            chosen = -DPO_BETA * pair_weight * masks[0][1] - scale * masks[0][1]
            rejected = DPO_BETA * pair_weight * masks[1][1]
            mine = jnp.where(tensor == 0, chosen, rejected)
            theirs = jnp.where(tensor == 0, rejected, chosen)
            rows = pl.ds(pl.multiple_of((2 * pair + tensor) * LENGTH, LENGTH), LENGTH)
            upstream[rows, :] = (mine * head_own[pair].astype(F32)).astype(BF)
            if pair == 0:
                kept = theirs
        send_head.wait_recv()
        for pair, theirs in enumerate((kept, theirs)):
            rows = pl.ds(pl.multiple_of((2 * pair + 1 - tensor) * LENGTH, LENGTH), LENGTH)
            upstream[rows, :] = (theirs * head_other[pair].astype(F32)).astype(BF)
        send_weight.start()

    @pl.when(pipe == 0)
    def _():
        pl.semaphore_wait(go, 1)
        send_weight.start()
        for send in send_below:
            send.wait_recv()

    def heads_back(first, count):
        rows = pl.ds(pl.multiple_of(first * 128, 128), count * 128)
        block = lax.dot_general(
            upstream[...], weight_out[rows, :], (((1,), (1,)), ((), ())), preferred_element_type=F32
        ).astype(BF)
        for head in range(count):
            at = pl.ds(pl.multiple_of((first + head) * LENGTH, LENGTH), LENGTH)
            for index in range(4):
                mixed_grad[index, at, :] = block[
                    index * LENGTH : (index + 1) * LENGTH, head * 128 : (head + 1) * 128
                ]

    def two_heads(index, carry):
        heads_back(2 * index, 2)
        return carry

    lax.fori_loop(0, 3, two_heads, 0)
    heads_back(6, 1)

    @pl.when(pipe == 1)
    def _():
        pl.semaphore_signal(go, inc=1, device_id=partner, device_id_type=MESH)

    def unmix(index, carry):
        rows = pl.ds(pl.multiple_of(index * LENGTH, LENGTH), LENGTH)
        grad[rows, :] = lax.dot_general(
            pattern[index], mixed_grad[index], (((0,), (0,)), ((), ())), preferred_element_type=F32
        ).astype(BF)
        return carry

    lax.fori_loop(0, 4, unmix, 0)
    send_grad.start()

    def products(index, carry):
        at = pl.ds(pl.multiple_of(index * 896, 128), 896)
        places = pl.ds(2 * index, 2)
        turned = upstream[:, at].T
        block = jnp.dot(turned, mixed[:, :COLS], preferred_element_type=F32).astype(BF)
        part_a[places] = block.reshape(2, 4, 112, COLS)
        block = jnp.dot(turned, mixed[:, COLS:], preferred_element_type=F32).astype(BF)
        part_b[places, :, :, : COLS - HEAD_DIM] = block.reshape(2, 4, 112, COLS - HEAD_DIM)
        block = jnp.dot(normed[:, at].T, grad[...], preferred_element_type=F32).astype(BF)
        part_b[places, :, :, COLS - HEAD_DIM :] = block.reshape(2, 4, 112, HEAD_DIM)
        return carry

    lax.fori_loop(0, 4, products, 0)

    def flow(size, place, ways, local, landing, hops):
        nonlocal base
        first = base
        made = Flow(
            size, place, *ways, local, lambda slot: landing.at[slot - first], sends, receives, base, hops
        )
        base += made.count
        return made

    z_halves = {(1, 0): 4, (-1, 1): 4, (1, 1): 3, (-1, 0): 3}
    y_halves = {(1, 0): 2, (-1, 1): 2, (1, 1): 1, (-1, 0): 1}
    z_whole = {(1, 0): 4, (-1, 0): 3}
    y_whole = {(1, 0): 2, (-1, 0): 1}
    a1 = flow(8, z, z_ways, lambda q, h: part_a.at[q, pl.ds(2 * h, 2)], land_a1, z_halves)
    b1 = flow(4, y, y_ways, lambda q, h: part_b.at[pl.ds(4 * h, 4), q], land_b1, y_halves)
    a2 = flow(4, y, y_ways, lambda q, h: part_a.at[z, q], land_a2, y_whole)
    b2 = flow(8, z, z_ways, lambda q, h: part_b.at[q, y], land_b2, z_whole)
    g1 = flow(8, z, z_ways, lambda q, h: part_g.at[q], land_g1, z_whole)
    g2 = flow(4, y, y_ways, lambda q, h: part_g.at[z, q], land_g2, y_whole)

    a1.step(0)
    b1.step(0)
    send_weight.wait_recv()
    send_grad.wait_recv()

    def norm_back(index, total):
        at = pl.ds(pl.multiple_of(index * BLOCK, BLOCK), BLOCK)
        last_dims = (((1,), (1,)), ((), ()))
        mine = lax.dot_general(grad[...], weight[at, :], last_dims, preferred_element_type=F32)
        theirs = lax.dot_general(
            grad_other[...], weight_other[at, :], last_dims, preferred_element_type=F32
        )
        both = mine.astype(BF).astype(F32) + theirs.astype(BF).astype(F32)
        normed_grad[:, at] = both
        term = both * inputs[:, at].astype(F32)
        gain_row[:, at] = jnp.sum(term * wide(rms[...]), axis=0, keepdims=True)
        term = term * gain[:, at]
        return total + term[:, :128] + term[:, 128:]

    total = lax.fori_loop(0, BLOCKS, norm_back, jnp.zeros((TOKENS, 128), F32))
    mean = jnp.sum(total, axis=1, keepdims=True) / WIDTH
    cubed = rms[...] * rms[...] * rms[...] * mean
    normed_grad_scale = cubed
    outputs = []
    for pair in range(2):
        rows = pl.ds(128 * pair, 128)
        slope = wide(normed_grad_scale[128 * pair : 128 * (pair + 1)])

        def through(index, carry):
            at = pl.ds(pl.multiple_of(index * BLOCK, BLOCK), BLOCK)
            scaled = normed_grad[rows, at] * gain[:, at]
            change = wide(rms[rows, :]) * scaled - inputs[rows, at].astype(F32) * slope
            below[rows, at] = (upstream[rows, at].astype(F32) + change).astype(BF)
            return carry

        lax.fori_loop(0, BLOCKS, through, 0)

        @pl.when(pipe == 1)
        def _():
            send_below[pair].start()

        own = pl.ds(pl.multiple_of((2 * pair + tensor) * LENGTH, LENGTH), LENGTH)
        output = pltpu.make_async_copy(below.at[own], cotangent_out.at[pair], load_sems.at[5 + pair])
        output.start()
        outputs.append(output)

    for place in range(32):
        part_g[place // 4, place % 4, :, :112] = gain_row[:, 112 * place : 112 * (place + 1)]

    def last(index, source, target):
        return pltpu.make_async_remote_copy(
            src_ref=source,
            dst_ref=target,
            send_sem=sends.at[base + index],
            recv_sem=receives.at[base + index],
            device_id=x_way,
            device_id_type=MESH,
        )

    def exchange(index, part):
        total = part[z, y].astype(F32)
        low, high = total[:56], total[56:]
        last_src[index] = jnp.where(x == 0, high, low).astype(BF)
        copy = last(index, last_src.at[index], last_dst.at[index])
        copy.start()
        return copy, jnp.where(x == 0, low, high)

    a1.step(1)
    g1.step(0)
    b1.step(1)
    g1.step(1)
    a1.step(2)
    g1.step(2)
    a1.step(3)
    g1.step(3)
    b1.finish()
    b2.step(0)
    a1.finish()
    a2.step(0)
    g1.finish()
    g2.step(0)
    b2.step(1)
    a2.step(1)
    g2.step(1)
    b2.step(2)
    a2.finish()
    copy_a, own_a = exchange(0, part_a)
    mixed_out[:, :COLS] = own_a
    g2.finish()
    copy_g = last(2, part_g.at[z, y], last_g)
    copy_g.start()
    b2.step(3)
    b2.finish()
    copy_b, own_b = exchange(1, part_b)
    mixed_out[:, COLS:] = own_b[:, : COLS - HEAD_DIM]
    value_out[...] = own_b[:, COLS - HEAD_DIM :]
    copy_a.wait_recv()
    mixed_out[:, :COLS] += last_dst[0].astype(F32)
    copy_g.wait_recv()
    gain_total = part_g[z, y] + last_g[...]
    gain_out[...] = jnp.where(x == 0, gain_total[:, :56], gain_total[:, 56:112])
    copy_b.wait_recv()
    landed = last_dst[1].astype(F32)
    mixed_out[:, COLS:] += landed[:, : COLS - HEAD_DIM]
    value_out[...] += landed[:, COLS - HEAD_DIM :]
    for made in (count_z, count_y, count_x, a1, b1, a2, b2, g1, g2):
        made.drain()
    for copy in (copy_a, copy_b, copy_g, send_weight, send_grad):
        copy.wait_send()
    for output in outputs:
        output.wait()

    @pl.when(pipe == 1)
    def _():
        send_head.wait_send()
        for send in send_below:
            send.wait_send()


def body(
    hidden_in,
    attention_probs,
    norm_gain,
    value_weight,
    output_weight,
    head_grad,
    policy_logprob,
    reference_logprob,
    sequence_bounds,
):
    copies = 7 + 3 + 1 + 14 + 6 + 3 + 7 + 7 + 3 + 3
    vmem = pl.BlockSpec(memory_space=pltpu.VMEM)
    smem = pl.BlockSpec(memory_space=pltpu.SMEM)
    hbm = pl.BlockSpec(memory_space=pl.ANY)
    mixed_share, value_share, gain_share, own_output = pl.pallas_call(
        step_kernel,
        out_shape=(
            jax.ShapeDtypeStruct((56, HEADS * HEAD_DIM), F32),
            jax.ShapeDtypeStruct((56, HEAD_DIM), F32),
            jax.ShapeDtypeStruct((1, 56), F32),
            jax.ShapeDtypeStruct((2, LENGTH, WIDTH), BF),
        ),
        in_specs=[smem, smem, vmem, vmem, hbm, hbm, hbm, hbm, hbm],
        out_specs=(vmem, vmem, vmem, hbm),
        scratch_shapes=[
            pltpu.VMEM((TOKENS, WIDTH), BF),
            pltpu.VMEM((4, HEADS * LENGTH, LENGTH), BF),
            pltpu.VMEM((WIDTH, HEAD_DIM), BF),
            pltpu.VMEM((WIDTH, HEAD_DIM), BF),
            pltpu.VMEM((HEADS * HEAD_DIM, WIDTH), BF),
            pltpu.VMEM((2, LENGTH, WIDTH), BF),
            pltpu.VMEM((2, LENGTH, WIDTH), BF),
            pltpu.VMEM((TOKENS, WIDTH), BF),
            pltpu.VMEM((TOKENS, WIDTH), BF),
            pltpu.VMEM((TOKENS, WIDTH), BF),
            pltpu.VMEM((TOKENS, HEAD_DIM), BF),
            pltpu.VMEM((TOKENS, HEADS * HEAD_DIM), BF),
            pltpu.VMEM((4, HEADS * LENGTH, HEAD_DIM), BF),
            pltpu.VMEM((TOKENS, HEAD_DIM), BF),
            pltpu.VMEM((TOKENS, HEAD_DIM), BF),
            pltpu.VMEM((TOKENS, WIDTH), F32),
            pltpu.VMEM((TOKENS, 128), F32),
            pltpu.VMEM((1, WIDTH), F32),
            pltpu.VMEM((3, 1, 128), F32),
            pltpu.VMEM((7, 1, 128), F32),
            pltpu.VMEM((3, 1, 128), F32),
            pltpu.VMEM((1, 1, 128), F32),
            pltpu.VMEM((8, 4, 112, COLS), BF),
            pltpu.VMEM((8, 4, 112, COLS), BF),
            pltpu.VMEM((8, 4, 1, 128), F32),
            pltpu.VMEM((14, 2, 112, COLS), BF),
            pltpu.VMEM((6, 4, 112, COLS), BF),
            pltpu.VMEM((3, 112, COLS), BF),
            pltpu.VMEM((7, 112, COLS), BF),
            pltpu.VMEM((7, 4, 1, 128), F32),
            pltpu.VMEM((3, 1, 128), F32),
            pltpu.VMEM((2, 56, COLS), BF),
            pltpu.VMEM((2, 56, COLS), BF),
            pltpu.VMEM((1, 128), F32),
            pltpu.SemaphoreType.DMA((7,)),
            pltpu.SemaphoreType.DMA((5,)),
            pltpu.SemaphoreType.DMA((5,)),
            pltpu.SemaphoreType.REGULAR,
            pltpu.SemaphoreType.DMA((copies,)),
            pltpu.SemaphoreType.DMA((copies,)),
        ],
        compiler_params=pltpu.CompilerParams(
            collective_id=0, has_side_effects=True, vmem_limit_bytes=60 * 1024 * 1024
        ),
    )(
        sequence_bounds,
        reference_logprob,
        policy_logprob,
        norm_gain,
        hidden_in.reshape(TOKENS, WIDTH),
        attention_probs.reshape(4, HEADS * LENGTH, LENGTH),
        value_weight[0],
        output_weight[0],
        head_grad.reshape(2, LENGTH, WIDTH),
    )
    return (
        own_output.reshape(1, 2, 1, LENGTH, WIDTH),
        value_share[None],
        mixed_share[None],
        gain_share,
    )


def solution(mesh):
    in_specs = (
        P("pipe", "dp", None, None, None),
        P("pipe", "dp", None, "tensor", None, None),
        P("pipe", None),
        P("pipe", None, "tensor"),
        P("pipe", "tensor", None),
        P("dp", "tensor", None, None),
        P("dp", None, None),
        P("dp", None),
        P("dp", None),
    )
    out_specs = (
        P("pipe", "dp", "tensor", None, None),
        P("pipe", "dp", "tensor"),
        P("pipe", "dp", "tensor"),
        P("pipe", "dp"),
    )
    return jax.shard_map(body, mesh=mesh, in_specs=in_specs, out_specs=out_specs, check_vma=False)
```

```python
import functools

import jax
import jax.numpy as jnp
from jax import lax
from jax.experimental import pallas as pl
from jax.experimental.pallas import tpu as pltpu
from jax.sharding import PartitionSpec as P

HEAD_DIM = 128
EPSILON = 1e-06
DPO_BETA = 0.25
LIKELIHOOD_COEF = 0.2
MESH = pl.DeviceIdType.MESH
BF = jnp.bfloat16
F32 = jnp.float32
COLS = 512
SPLIT = 384


class Flow:
    def __init__(self, size, place, ahead, behind, local, landing, sends, receives, base, hops):
        self.size, self.place = size, place
        self.target = {1: ahead, -1: behind}
        self.local, self.landing = local, landing
        self.sends, self.receives = sends, receives
        self.hops = hops
        self.slot = {}
        for (way, half), count in hops.items():
            for step in range(count):
                self.slot[way, half, step] = base + len(self.slot)
        self.count = len(self.slot)
        self.copies = {}

    def copy(self, way, half, step):
        slot = self.slot[way, half, step]
        chunk = lax.rem(self.place + way * (self.hops[way, half] - step) + self.size, self.size)
        source = self.local(chunk, half)
        return chunk, pltpu.make_async_remote_copy(
            src_ref=source,
            dst_ref=self.landed(slot, source),
            send_sem=self.sends.at[slot],
            recv_sem=self.receives.at[slot],
            device_id=self.target[way],
            device_id_type=MESH,
        )

    def landed(self, slot, like):
        landing = self.landing(slot)
        if landing.shape == like.shape:
            return landing
        return landing.at[pl.ds(0, like.shape[0])]

    def collect(self, way, half, step, chunk):
        self.copies[way, half, step].wait_recv()
        target = self.local(chunk, half)
        add_into(target, self.landed(self.slot[way, half, step], target))

    def step(self, step):
        for way, half in self.hops:
            if step < self.hops[way, half]:
                chunk, copy = self.copy(way, half, step)
                if step:
                    self.collect(way, half, step - 1, chunk)
                copy.start()
                self.copies[way, half, step] = copy

    def finish(self):
        for (way, half), count in self.hops.items():
            self.collect(way, half, count - 1, self.place)

    def drain(self):
        for copy in self.copies.values():
            copy.wait_send()


def add_into(target, landed):
    if len(target.shape) > 2 and target.shape[-2] > 1:

        def one(index, carry):
            target[index] = target[index] + landed[index]
            return carry

        lax.fori_loop(0, target.shape[0], one, 0)
    else:
        target[...] = target[...] + landed[...]


class Spread:
    def __init__(self, size, place, device_at, own, landing, sends, receives, base):
        self.own, self.landing = own, landing
        self.count = size - 1
        self.copies = [
            pltpu.make_async_remote_copy(
                src_ref=own,
                dst_ref=landing.at[slot],
                send_sem=sends.at[base + slot],
                recv_sem=receives.at[base + slot],
                device_id=device_at(lax.rem(place + 1 + slot, size)),
                device_id_type=MESH,
            )
            for slot in range(self.count)
        ]

    def start(self):
        for copy in self.copies:
            copy.start()

    def finish(self):
        total = self.own[...]
        for slot, copy in enumerate(self.copies):
            copy.wait_recv()
            total = total + self.landing[slot]
        return total

    def drain(self):
        for copy in self.copies:
            copy.wait_send()


WIDTH = 3584
TOKENS = 256
BLOCK = 256
BLOCKS = WIDTH // BLOCK
LENGTH = 64
HEADS = 7


def wide(rows):
    return jnp.concatenate([rows, rows], axis=1)


def step_kernel(
    bounds,
    reference,
    logprob,
    gain,
    inputs_hbm,
    pattern_hbm,
    value_hbm,
    output_hbm,
    head_hbm,
    mixed_out,
    value_out,
    gain_out,
    cotangent_out,
    inputs,
    pattern,
    weight,
    weight_other,
    weight_out,
    head_own,
    head_other,
    upstream,
    upstream_turned,
    below,
    normed,
    values,
    mixed,
    mixed_grad,
    grad,
    grad_other,
    normed_grad,
    rms,
    gain_row,
    counts,
    land_cz,
    land_cy,
    land_cx,
    part_a,
    part_b,
    part_g,
    land_a1,
    land_b1,
    land_a2,
    land_b2,
    land_g1,
    land_g2,
    last_src,
    last_dst,
    last_g,
    load_sems,
    pass_sends,
    pass_receives,
    go,
    sends,
    receives,
):
    pipe = lax.axis_index("pipe")
    tensor = lax.axis_index("tensor")
    dp = lax.axis_index("dp")
    z = dp // 8
    y = lax.rem(dp, 8) // 2
    x = lax.rem(dp, 2)

    def device(z_at, y_at, x_at):
        return (pipe, z_at * 8 + y_at * 2 + x_at, tensor)

    z_next, z_prev = lax.rem(z + 1, 8), lax.rem(z + 7, 8)
    y_next, y_prev = lax.rem(y + 1, 4), lax.rem(y + 3, 4)
    z_ways = (device(z_next, y, x), device(z_prev, y, x))
    y_ways = (device(z, y_next, x), device(z, y_prev, x))
    x_way = device(z, y, 1 - x)
    peer = (pipe, dp, 1 - tensor)
    cross = (pipe, z * 8 + y * 2 + 1 - x, 1 - tensor)
    partner = (1 - pipe, dp, tensor)

    loads = {
        name: pltpu.make_async_copy(source, target, load_sems.at[index])
        for index, (name, source, target) in enumerate(
            (
                ("inputs", inputs_hbm, inputs),
                ("weight", value_hbm, weight),
                ("pattern", pattern_hbm, pattern),
                ("head", head_hbm, head_own),
                ("output", output_hbm, weight_out),
            )
        )
    }
    for load in loads.values():
        load.start()

    def token_rows(pair, which):
        lanes = lax.broadcasted_iota(jnp.int32, (1, LENGTH), 1)
        rows = lax.broadcasted_iota(jnp.int32, (LENGTH, 1), 0)
        first, end = bounds[pair, 0], bounds[pair, 1 + which]
        row_mask = ((lanes >= first) & (lanes < end)).astype(F32)
        column_mask = ((rows >= first) & (rows < end)).astype(F32)
        return row_mask, column_mask

    own_count = jnp.zeros((1, 1), F32)
    for pair in range(2):
        own_count = own_count + jnp.sum(token_rows(pair, 0)[0], axis=1, keepdims=True)
    counts[0] = jnp.broadcast_to(own_count, (1, 128))
    part_g[...] = jnp.zeros_like(part_g)

    barrier = pltpu.get_barrier_semaphore()
    z_others = [device(lax.rem(z + step, 8), y, x) for step in range(1, 8)]
    y_others = [device(z, lax.rem(y + step, 4), x) for step in range(1, 4)]
    for neighbour in (*z_others, *y_others, x_way, peer, cross, partner):
        pl.semaphore_signal(barrier, inc=1, device_id=neighbour, device_id_type=MESH)
    pl.semaphore_wait(barrier, 14)

    def passing(index, source, target, to):
        return pltpu.make_async_remote_copy(
            src_ref=source,
            dst_ref=target,
            send_sem=pass_sends.at[index],
            recv_sem=pass_receives.at[index],
            device_id=to,
            device_id_type=MESH,
        )

    send_head = passing(0, head_hbm, head_other, peer)
    send_weight = passing(1, value_hbm, weight_other, cross)
    send_grad = passing(2, grad, grad_other, peer)
    send_below = [
        passing(3 + pair, below.at[pl.ds(128 * pair, 128)], upstream.at[pl.ds(128 * pair, 128)], partner)
        for pair in range(2)
    ]

    @pl.when(pipe == 1)
    def _():
        send_head.start()

    base = 0

    def spread(size, place, device_at, own, landing):
        nonlocal base
        made = Spread(size, place, device_at, own, landing, sends, receives, base)
        base += made.count
        return made

    count_z = spread(8, z, lambda at: device(at, y, x), counts.at[0], land_cz)
    count_y = spread(4, y, lambda at: device(z, at, x), counts.at[1], land_cy)
    count_x = spread(2, x, lambda at: device(z, y, at), counts.at[2], land_cx)

    count_z.start()
    loads["inputs"].wait()

    def square(index, total):
        at = pl.ds(pl.multiple_of(index * BLOCK, BLOCK), BLOCK)
        block = inputs[:, at].astype(F32)
        block = block * block
        return total + block[:, :128] + block[:, 128:]

    total = lax.fori_loop(0, BLOCKS, square, jnp.zeros((TOKENS, 128), F32))
    mean = jnp.sum(total, axis=1, keepdims=True) / WIDTH
    rms[...] = jnp.broadcast_to(lax.rsqrt(mean + EPSILON), (TOKENS, 128))
    loads["weight"].wait()

    def project(index, total):
        at = pl.ds(pl.multiple_of(index * BLOCK, BLOCK), BLOCK)
        block = (inputs[:, at].astype(F32) * wide(rms[...]) * gain[:, at]).astype(BF)
        normed[:, at] = block
        return total + jnp.dot(block, weight[at, :], preferred_element_type=F32)

    total = lax.fori_loop(0, BLOCKS, project, jnp.zeros((TOKENS, 128), F32))
    values[...] = total.astype(BF)
    counts[1] = count_z.finish()
    count_y.start()
    loads["pattern"].wait()

    def mix(index, carry):
        rows = pl.ds(pl.multiple_of(index * LENGTH, LENGTH), LENGTH)
        block = jnp.dot(pattern[index], values[rows, :], preferred_element_type=F32).astype(BF)
        for head in range(HEADS):
            mixed[rows, head * 128 : (head + 1) * 128] = block[head * LENGTH : (head + 1) * LENGTH]
        return carry

    lax.fori_loop(0, 2, mix, 0)
    counts[2] = count_y.finish()
    count_x.start()
    lax.fori_loop(2, 4, mix, 0)
    loads["head"].wait()
    total_count = count_x.finish()[:, :1]
    loads["output"].wait()

    @pl.when(pipe == 1)
    def _():
        scale = jnp.full((1, 1), LIKELIHOOD_COEF * 128, F32) / total_count
        for pair in range(2):
            masks = [token_rows(pair, which) for which in range(2)]
            sums = [
                jnp.sum(masks[which][0] * logprob[pair, which : which + 1, :], axis=1, keepdims=True)
                for which in range(2)
            ]
            margin = DPO_BETA * (
                sums[0] - reference[pair, 0] - (sums[1] - reference[pair, 1])
            )
            pair_weight = jax.nn.sigmoid(-margin)
            chosen = -DPO_BETA * pair_weight * masks[0][1] - scale * masks[0][1]
            rejected = DPO_BETA * pair_weight * masks[1][1]
            mine = jnp.where(tensor == 0, chosen, rejected)
            theirs = jnp.where(tensor == 0, rejected, chosen)
            rows = pl.ds(pl.multiple_of((2 * pair + tensor) * LENGTH, LENGTH), LENGTH)
            upstream[rows, :] = (mine * head_own[pair].astype(F32)).astype(BF)
            if pair == 0:
                kept = theirs
        send_head.wait_recv()
        send_weight.start()
        for pair, theirs in enumerate((kept, theirs)):
            rows = pl.ds(pl.multiple_of((2 * pair + 1 - tensor) * LENGTH, LENGTH), LENGTH)
            upstream[rows, :] = (theirs * head_other[pair].astype(F32)).astype(BF)

    @pl.when(pipe == 0)
    def _():
        pl.semaphore_wait(go, 1)
        send_weight.start()
        for send in send_below:
            send.wait_recv()

    def flow(size, place, ways, local, landing, hops):
        nonlocal base
        first = base
        made = Flow(
            size, place, *ways, local, lambda slot: landing.at[slot - first], sends, receives, base, hops
        )
        base += made.count
        return made

    z_halves = {(1, 0): 4, (-1, 1): 4, (1, 1): 3, (-1, 0): 3}
    y_halves = {(1, 0): 2, (-1, 1): 2, (1, 1): 1, (-1, 0): 1}
    z_whole = {(1, 0): 4, (-1, 0): 3}
    y_whole = {(1, 0): 2, (-1, 0): 1}
    rows_of = (pl.ds(0, 64), pl.ds(64, 48))
    a1 = flow(8, z, z_ways, lambda q, h: part_a.at[q, pl.ds(2 * h, 2)], land_a1, z_halves)
    b1 = flow(4, y, y_ways, lambda q, h: part_b.at[pl.ds(4 * h, 4), q], land_b1, y_halves)
    a2 = flow(4, y, y_ways, lambda q, h: part_a.at[z, q, rows_of[h]], land_a2, y_halves)
    b2 = flow(8, z, z_ways, lambda q, h: part_b.at[q, y, rows_of[h]], land_b2, z_halves)
    g1 = flow(8, z, z_ways, lambda q, h: part_g.at[q], land_g1, z_whole)
    g2 = flow(4, y, y_ways, lambda q, h: part_g.at[z, q], land_g2, y_whole)

    def later_products(index, carry):
        at = pl.ds(pl.multiple_of(index * 896, 128), 896)
        rows = pl.ds(pl.multiple_of(index * 896, 128), 896)
        places = pl.ds(2 * index, 2)
        upstream_turned[rows, :] = upstream[:, at].T
        block = jnp.dot(upstream_turned[rows, :], mixed[:, SPLIT:], preferred_element_type=F32)
        part_b[places] = block.astype(BF).reshape(2, 4, 112, COLS)
        return carry

    lax.fori_loop(0, 4, later_products, 0)
    b1.step(0)

    def heads_back(first, count):
        rows = pl.ds(pl.multiple_of(first * 128, 128), count * 128)
        block = lax.dot_general(
            upstream[...], weight_out[rows, :], (((1,), (1,)), ((), ())), preferred_element_type=F32
        ).astype(BF)
        for head in range(count):
            at = pl.ds(pl.multiple_of((first + head) * LENGTH, LENGTH), LENGTH)
            for index in range(4):
                mixed_grad[index, at, :] = block[
                    index * LENGTH : (index + 1) * LENGTH, head * 128 : (head + 1) * 128
                ]

    def two_heads(index, carry):
        heads_back(2 * index, 2)
        return carry

    lax.fori_loop(0, 3, two_heads, 0)
    heads_back(6, 1)

    @pl.when(pipe == 1)
    def _():
        pl.semaphore_signal(go, inc=1, device_id=partner, device_id_type=MESH)

    def unmix(index, carry):
        rows = pl.ds(pl.multiple_of(index * LENGTH, LENGTH), LENGTH)
        grad[rows, :] = lax.dot_general(
            pattern[index], mixed_grad[index], (((0,), (0,)), ((), ())), preferred_element_type=F32
        ).astype(BF)
        return carry

    lax.fori_loop(0, 4, unmix, 0)
    send_grad.start()

    def first_products(index, carry):
        at = pl.ds(pl.multiple_of(index * 896, 128), 896)
        rows = pl.ds(pl.multiple_of(index * 896, 128), 896)
        places = pl.ds(2 * index, 2)
        block = jnp.dot(upstream_turned[rows, :], mixed[:, :SPLIT], preferred_element_type=F32)
        part_a[places, :, :, :SPLIT] = block.astype(BF).reshape(2, 4, 112, SPLIT)
        block = jnp.dot(normed[:, at].T, grad[...], preferred_element_type=F32)
        part_a[places, :, :, SPLIT:] = block.astype(BF).reshape(2, 4, 112, HEAD_DIM)
        return carry

    lax.fori_loop(0, 4, first_products, 0)
    a1.step(0)
    send_weight.wait_recv()
    send_grad.wait_recv()

    outputs = []
    for pair in range(2):
        rows = pl.ds(128 * pair, 128)

        def norm_back(index, total):
            at = pl.ds(pl.multiple_of(index * BLOCK, BLOCK), BLOCK)
            last_dims = (((1,), (1,)), ((), ()))
            mine = lax.dot_general(
                grad[rows, :], weight[at, :], last_dims, preferred_element_type=F32
            )
            theirs = lax.dot_general(
                grad_other[rows, :], weight_other[at, :], last_dims, preferred_element_type=F32
            )
            both = mine.astype(BF).astype(F32) + theirs.astype(BF).astype(F32)
            normed_grad[rows, at] = both
            term = both * inputs[rows, at].astype(F32)
            terms = jnp.sum(term * wide(rms[rows, :]), axis=0, keepdims=True)
            gain_row[:, at] = terms if pair == 0 else gain_row[:, at] + terms
            term = term * gain[:, at]
            return total + term[:, :128] + term[:, 128:]

        total = lax.fori_loop(0, BLOCKS, norm_back, jnp.zeros((128, 128), F32))
        mean = jnp.sum(total, axis=1, keepdims=True) / WIDTH
        scale = rms[rows, :]
        slope = wide(scale * scale * scale * mean)

        def through(index, carry):
            at = pl.ds(pl.multiple_of(index * BLOCK, BLOCK), BLOCK)
            scaled = normed_grad[rows, at] * gain[:, at]
            change = wide(rms[rows, :]) * scaled - inputs[rows, at].astype(F32) * slope
            below[rows, at] = (upstream[rows, at].astype(F32) + change).astype(BF)
            return carry

        lax.fori_loop(0, BLOCKS, through, 0)

        @pl.when(pipe == 1)
        def _():
            send_below[pair].start()

        own = pl.ds(pl.multiple_of((2 * pair + tensor) * LENGTH, LENGTH), LENGTH)
        output = pltpu.make_async_copy(below.at[own], cotangent_out.at[pair], load_sems.at[5 + pair])
        output.start()
        outputs.append(output)

    for place in range(32):
        part_g[place // 4, place % 4, :, :112] = gain_row[:, 112 * place : 112 * (place + 1)]

    def last(index, source, target):
        return pltpu.make_async_remote_copy(
            src_ref=source,
            dst_ref=target,
            send_sem=sends.at[base + index],
            recv_sem=receives.at[base + index],
            device_id=x_way,
            device_id_type=MESH,
        )

    def exchange(index, part):
        total = part[z, y].astype(F32)
        low, high = total[:56], total[56:]
        last_src[index] = jnp.where(x == 0, high, low).astype(BF)
        copy = last(index, last_src.at[index], last_dst.at[index])
        copy.start()
        return copy, jnp.where(x == 0, low, high)

    g1.step(0)
    a1.step(1)
    b1.step(1)
    a1.step(2)
    g1.step(1)
    a1.step(3)
    g1.step(2)
    b1.finish()
    b2.step(0)
    a1.finish()
    a2.step(0)
    g1.step(3)
    b2.step(1)
    a2.step(1)
    g1.finish()
    g2.step(0)
    b2.step(2)
    a2.finish()
    copy_a, own_a = exchange(0, part_a)
    mixed_out[:, :SPLIT] = own_a[:, :SPLIT]
    value_out[...] = own_a[:, SPLIT:]
    g2.step(1)
    b2.step(3)
    g2.finish()
    copy_g = last(2, part_g.at[z, y], last_g)
    copy_g.start()
    b2.finish()
    copy_b, own_b = exchange(1, part_b)
    mixed_out[:, SPLIT:] = own_b
    copy_a.wait_recv()
    landed = last_dst[0].astype(F32)
    mixed_out[:, :SPLIT] += landed[:, :SPLIT]
    value_out[...] += landed[:, SPLIT:]
    copy_g.wait_recv()
    gain_total = part_g[z, y] + last_g[...]
    gain_out[...] = jnp.where(x == 0, gain_total[:, :56], gain_total[:, 56:112])
    copy_b.wait_recv()
    mixed_out[:, SPLIT:] += last_dst[1].astype(F32)
    for made in (count_z, count_y, count_x, a1, b1, a2, b2, g1, g2):
        made.drain()
    for copy in (copy_a, copy_b, copy_g, send_weight, send_grad):
        copy.wait_send()
    for output in outputs:
        output.wait()

    @pl.when(pipe == 1)
    def _():
        send_head.wait_send()
        for send in send_below:
            send.wait_send()


def copy_kernel(*refs):
    sources, targets, sems = refs[:4], refs[4:8], refs[8]
    copies = [
        pltpu.make_async_copy(source, target, sems.at[index])
        for index, (source, target) in enumerate(zip(sources, targets))
    ]
    for copy in copies:
        copy.start()
    for copy in copies:
        copy.wait()


def written_out(arrays):
    vmem = pl.BlockSpec(memory_space=pltpu.VMEM)
    hbm = pl.BlockSpec(memory_space=pl.ANY)
    return pl.pallas_call(
        copy_kernel,
        out_shape=tuple(jax.ShapeDtypeStruct(array.shape, array.dtype) for array in arrays),
        in_specs=[vmem] * 4,
        out_specs=(hbm,) * 4,
        scratch_shapes=[pltpu.SemaphoreType.DMA((4,))],
        compiler_params=pltpu.CompilerParams(vmem_limit_bytes=4 * 1024 * 1024),
    )(*arrays)


def body(
    hidden_in,
    attention_probs,
    norm_gain,
    value_weight,
    output_weight,
    head_grad,
    policy_logprob,
    reference_logprob,
    sequence_bounds,
):
    copies = 7 + 3 + 1 + 14 + 6 + 6 + 14 + 7 + 3 + 3
    vmem = pl.BlockSpec(memory_space=pltpu.VMEM)
    smem = pl.BlockSpec(memory_space=pltpu.SMEM)
    hbm = pl.BlockSpec(memory_space=pltpu.HBM)
    mixed_share, value_share, gain_share, own_output = pl.pallas_call(
        step_kernel,
        out_shape=(
            jax.ShapeDtypeStruct((56, HEADS * HEAD_DIM), F32),
            jax.ShapeDtypeStruct((56, HEAD_DIM), F32),
            jax.ShapeDtypeStruct((1, 56), F32),
            jax.ShapeDtypeStruct((2, LENGTH, WIDTH), BF),
        ),
        in_specs=[smem, smem, vmem, vmem, hbm, hbm, hbm, hbm, hbm],
        out_specs=(vmem, vmem, vmem, pl.BlockSpec(memory_space=pl.ANY)),
        scratch_shapes=[
            pltpu.VMEM((TOKENS, WIDTH), BF),
            pltpu.VMEM((4, HEADS * LENGTH, LENGTH), BF),
            pltpu.VMEM((WIDTH, HEAD_DIM), BF),
            pltpu.VMEM((WIDTH, HEAD_DIM), BF),
            pltpu.VMEM((HEADS * HEAD_DIM, WIDTH), BF),
            pltpu.VMEM((2, LENGTH, WIDTH), BF),
            pltpu.VMEM((2, LENGTH, WIDTH), BF),
            pltpu.VMEM((TOKENS, WIDTH), BF),
            pltpu.VMEM((WIDTH, TOKENS), BF),
            pltpu.VMEM((TOKENS, WIDTH), BF),
            pltpu.VMEM((TOKENS, WIDTH), BF),
            pltpu.VMEM((TOKENS, HEAD_DIM), BF),
            pltpu.VMEM((TOKENS, HEADS * HEAD_DIM), BF),
            pltpu.VMEM((4, HEADS * LENGTH, HEAD_DIM), BF),
            pltpu.VMEM((TOKENS, HEAD_DIM), BF),
            pltpu.VMEM((TOKENS, HEAD_DIM), BF),
            pltpu.VMEM((TOKENS, WIDTH), F32),
            pltpu.VMEM((TOKENS, 128), F32),
            pltpu.VMEM((1, WIDTH), F32),
            pltpu.VMEM((3, 1, 128), F32),
            pltpu.VMEM((7, 1, 128), F32),
            pltpu.VMEM((3, 1, 128), F32),
            pltpu.VMEM((1, 1, 128), F32),
            pltpu.VMEM((8, 4, 112, COLS), BF),
            pltpu.VMEM((8, 4, 112, COLS), BF),
            pltpu.VMEM((8, 4, 1, 128), F32),
            pltpu.VMEM((14, 2, 112, COLS), BF),
            pltpu.VMEM((6, 4, 112, COLS), BF),
            pltpu.VMEM((6, 64, COLS), BF),
            pltpu.VMEM((14, 64, COLS), BF),
            pltpu.VMEM((7, 4, 1, 128), F32),
            pltpu.VMEM((3, 1, 128), F32),
            pltpu.VMEM((2, 56, COLS), BF),
            pltpu.VMEM((2, 56, COLS), BF),
            pltpu.VMEM((1, 128), F32),
            pltpu.SemaphoreType.DMA((7,)),
            pltpu.SemaphoreType.DMA((5,)),
            pltpu.SemaphoreType.DMA((5,)),
            pltpu.SemaphoreType.REGULAR,
            pltpu.SemaphoreType.DMA((copies,)),
            pltpu.SemaphoreType.DMA((copies,)),
        ],
        compiler_params=pltpu.CompilerParams(
            collective_id=0, has_side_effects=True, vmem_limit_bytes=60_000_000
        ),
    )(
        sequence_bounds,
        reference_logprob,
        policy_logprob,
        norm_gain,
        hidden_in.reshape(TOKENS, WIDTH),
        attention_probs.reshape(4, HEADS * LENGTH, LENGTH),
        value_weight[0],
        output_weight[0],
        head_grad.reshape(2, LENGTH, WIDTH),
    )
    mixed_share, value_share, gain_share, own_output = written_out(
        (mixed_share, value_share, gain_share, own_output)
    )
    return (
        own_output.reshape(1, 2, 1, LENGTH, WIDTH),
        value_share[None],
        mixed_share[None],
        gain_share,
    )


def solution(mesh):
    in_specs = (
        P("pipe", "dp", None, None, None),
        P("pipe", "dp", None, "tensor", None, None),
        P("pipe", None),
        P("pipe", None, "tensor"),
        P("pipe", "tensor", None),
        P("dp", "tensor", None, None),
        P("dp", None, None),
        P("dp", None),
        P("dp", None),
    )
    out_specs = (
        P("pipe", "dp", "tensor", None, None),
        P("pipe", "dp", "tensor"),
        P("pipe", "dp", "tensor"),
        P("pipe", "dp"),
    )
    return jax.shard_map(body, mesh=mesh, in_specs=in_specs, out_specs=out_specs, check_vma=False)
```

```python
import functools

import jax
import jax.numpy as jnp
from jax import lax
from jax.experimental import pallas as pl
from jax.experimental.pallas import tpu as pltpu
from jax.sharding import PartitionSpec as P

HEAD_DIM = 128
EPSILON = 1e-06
DPO_BETA = 0.25
LIKELIHOOD_COEF = 0.2
MESH = pl.DeviceIdType.MESH
BF = jnp.bfloat16
F32 = jnp.float32
COLS = 512
SPLIT = 384


class Flow:
    def __init__(self, size, place, ahead, behind, local, landing, sends, receives, base, hops):
        self.size, self.place = size, place
        self.target = {1: ahead, -1: behind}
        self.local, self.landing = local, landing
        self.sends, self.receives = sends, receives
        self.hops = hops
        self.slot = {}
        for (way, half), count in hops.items():
            for step in range(count):
                self.slot[way, half, step] = base + len(self.slot)
        self.count = len(self.slot)
        self.copies = {}

    def copy(self, way, half, step):
        slot = self.slot[way, half, step]
        chunk = lax.rem(self.place + way * (self.hops[way, half] - step) + self.size, self.size)
        source = self.local(chunk, half)
        return chunk, pltpu.make_async_remote_copy(
            src_ref=source,
            dst_ref=self.landed(slot, source),
            send_sem=self.sends.at[slot],
            recv_sem=self.receives.at[slot],
            device_id=self.target[way],
            device_id_type=MESH,
        )

    def landed(self, slot, like):
        landing = self.landing(slot)
        if landing.shape == like.shape:
            return landing
        return landing.at[pl.ds(0, like.shape[0])]

    def collect(self, way, half, step, chunk):
        self.copies[way, half, step].wait_recv()
        target = self.local(chunk, half)
        add_into(target, self.landed(self.slot[way, half, step], target))

    def step(self, step):
        for way, half in self.hops:
            if step < self.hops[way, half]:
                chunk, copy = self.copy(way, half, step)
                if step:
                    self.collect(way, half, step - 1, chunk)
                copy.start()
                self.copies[way, half, step] = copy

    def finish(self):
        for (way, half), count in self.hops.items():
            self.collect(way, half, count - 1, self.place)

    def drain(self):
        for copy in self.copies.values():
            copy.wait_send()


def add_into(target, landed):
    if len(target.shape) > 2 and target.shape[-2] > 1:

        def one(index, carry):
            target[index] = target[index] + landed[index]
            return carry

        lax.fori_loop(0, target.shape[0], one, 0)
    else:
        target[...] = target[...] + landed[...]


class Spread:
    def __init__(self, size, place, device_at, own, landing, sends, receives, base):
        self.own, self.landing = own, landing
        self.count = size - 1
        self.copies = [
            pltpu.make_async_remote_copy(
                src_ref=own,
                dst_ref=landing.at[slot],
                send_sem=sends.at[base + slot],
                recv_sem=receives.at[base + slot],
                device_id=device_at(lax.rem(place + 1 + slot, size)),
                device_id_type=MESH,
            )
            for slot in range(self.count)
        ]

    def start(self):
        for copy in self.copies:
            copy.start()

    def finish(self):
        total = self.own[...]
        for slot, copy in enumerate(self.copies):
            copy.wait_recv()
            total = total + self.landing[slot]
        return total

    def drain(self):
        for copy in self.copies:
            copy.wait_send()


class Shares(Spread):
    def __init__(self, size, place, device_at, local, landing, sends, receives, base):
        self.own, self.landing = local.at[place], landing
        self.count = size - 1
        self.copies = []
        for slot in range(self.count):
            at = lax.rem(place + 1 + slot, size)
            self.copies.append(
                pltpu.make_async_remote_copy(
                    src_ref=local.at[at],
                    dst_ref=landing.at[slot],
                    send_sem=sends.at[base + slot],
                    recv_sem=receives.at[base + slot],
                    device_id=device_at(at),
                    device_id_type=MESH,
                )
            )


WIDTH = 3584
TOKENS = 256
BLOCK = 256
BLOCKS = WIDTH // BLOCK
LENGTH = 64
HEADS = 7


def wide(rows):
    return jnp.concatenate([rows, rows], axis=1)


def step_kernel(
    bounds_hbm,
    reference_hbm,
    logprob_hbm,
    gain_hbm,
    inputs_hbm,
    pattern_hbm,
    value_hbm,
    output_hbm,
    head_hbm,
    kept_out,
    landed_out,
    gain_kept_out,
    gain_landed_out,
    cotangent_out,
    bounds,
    reference,
    logprob,
    gain,
    inputs,
    pattern,
    weight,
    weight_other,
    weight_out,
    head_own,
    head_other,
    upstream,
    upstream_turned,
    below,
    normed,
    values,
    mixed,
    mixed_grad,
    grad,
    grad_other,
    normed_grad,
    rms,
    slopes,
    gain_row,
    counts,
    land_cz,
    land_cy,
    land_cx,
    part_a,
    part_b,
    part_g,
    part_h,
    land_a1,
    land_v1,
    land_b1,
    land_a2,
    land_b2,
    land_g1,
    land_g2,
    last_src,
    kept,
    gain_last,
    gain_kept,
    load_sems,
    pass_sends,
    pass_receives,
    go,
    sends,
    receives,
):
    pipe = lax.axis_index("pipe")
    tensor = lax.axis_index("tensor")
    dp = lax.axis_index("dp")
    z = dp // 8
    y = lax.rem(dp, 8) // 2
    x = lax.rem(dp, 2)

    def device(z_at, y_at, x_at):
        return (pipe, z_at * 8 + y_at * 2 + x_at, tensor)

    z_next, z_prev = lax.rem(z + 1, 8), lax.rem(z + 7, 8)
    y_next, y_prev = lax.rem(y + 1, 4), lax.rem(y + 3, 4)
    z_ways = (device(z_next, y, x), device(z_prev, y, x))
    y_ways = (device(z, y_next, x), device(z, y_prev, x))
    x_way = device(z, y, 1 - x)
    peer = (pipe, dp, 1 - tensor)
    cross = (pipe, z * 8 + y * 2 + 1 - x, 1 - tensor)
    partner = (1 - pipe, dp, tensor)

    def token_rows(pair, which):
        lanes = lax.broadcasted_iota(jnp.int32, (1, LENGTH), 1)
        rows = lax.broadcasted_iota(jnp.int32, (LENGTH, 1), 0)
        first, end = bounds[pair, 0], bounds[pair, 1 + which]
        row_mask = ((lanes >= first) & (lanes < end)).astype(F32)
        column_mask = ((rows >= first) & (rows < end)).astype(F32)
        return row_mask, column_mask

    barrier = pltpu.get_barrier_semaphore()
    z_others = [device(lax.rem(z + step, 8), y, x) for step in range(1, 8)]
    y_others = [device(z, lax.rem(y + step, 4), x) for step in range(1, 4)]
    for neighbour in (*z_others, *y_others, x_way, peer, cross, partner):
        pl.semaphore_signal(barrier, inc=1, device_id=neighbour, device_id_type=MESH)
    loads = {
        name: pltpu.make_async_copy(source, target, load_sems.at[index])
        for index, (name, source, target) in enumerate(
            (
                ("head", head_hbm, head_own),
                ("bounds", bounds_hbm, bounds),
                ("reference", reference_hbm, reference),
                ("logprob", logprob_hbm, logprob),
                ("gain", gain_hbm, gain),
                ("inputs", inputs_hbm, inputs),
                ("weight", value_hbm, weight),
                ("pattern", pattern_hbm, pattern),
                ("output", output_hbm, weight_out),
            )
        )
    }
    for load in loads.values():
        load.start()

    for name in ("bounds", "reference", "logprob", "gain"):
        loads[name].wait()
    own_count = jnp.zeros((1, 1), F32)
    for pair in range(2):
        own_count = own_count + jnp.sum(token_rows(pair, 0)[0], axis=1, keepdims=True)
    counts[0] = jnp.broadcast_to(own_count, (1, 128))
    part_g[...] = jnp.zeros_like(part_g)
    gain_last[...] = jnp.zeros_like(gain_last)
    gain_kept[...] = jnp.zeros_like(gain_kept)
    pl.semaphore_wait(barrier, 14)
    loads["head"].wait()

    def passing(index, source, target, to):
        return pltpu.make_async_remote_copy(
            src_ref=source,
            dst_ref=target,
            send_sem=pass_sends.at[index],
            recv_sem=pass_receives.at[index],
            device_id=to,
            device_id_type=MESH,
        )

    send_head = passing(0, head_own, head_other, peer)
    send_weight = passing(1, weight, weight_other, cross)
    send_grad = passing(2, grad, grad_other, peer)
    send_below = [
        passing(3 + pair, below.at[pl.ds(128 * pair, 128)], upstream.at[pl.ds(128 * pair, 128)], partner)
        for pair in range(2)
    ]

    base = 0

    def spread(size, place, device_at, own, landing):
        nonlocal base
        made = Spread(size, place, device_at, own, landing, sends, receives, base)
        base += made.count
        return made

    count_x = spread(2, x, lambda at: device(z, y, at), counts.at[0], land_cx)
    count_z = spread(8, z, lambda at: device(at, y, x), counts.at[1], land_cz)
    count_y = spread(4, y, lambda at: device(z, at, x), counts.at[2], land_cy)
    count_x.start()

    @pl.when(pipe == 1)
    def _():
        send_head.start()

    loads["inputs"].wait()

    def square(index, total):
        at = pl.ds(pl.multiple_of(index * BLOCK, BLOCK), BLOCK)
        block = inputs[:, at].astype(F32)
        block = block * block
        return total + block[:, :128] + block[:, 128:]

    total = lax.fori_loop(0, BLOCKS, square, jnp.zeros((TOKENS, 128), F32))
    mean = jnp.sum(total, axis=1, keepdims=True) / WIDTH
    rms[...] = jnp.broadcast_to(lax.rsqrt(mean + EPSILON), (TOKENS, 128))
    counts[1] = count_x.finish()
    count_z.start()
    loads["weight"].wait()

    def project(index, total):
        at = pl.ds(pl.multiple_of(index * BLOCK, BLOCK), BLOCK)
        block = (inputs[:, at].astype(F32) * wide(rms[...]) * gain[:, at]).astype(BF)
        normed[:, at] = block
        return total + jnp.dot(block, weight[at, :], preferred_element_type=F32)

    total = lax.fori_loop(0, BLOCKS, project, jnp.zeros((TOKENS, 128), F32))
    values[...] = total.astype(BF)
    loads["pattern"].wait()

    def mix(index, carry):
        rows = pl.ds(pl.multiple_of(index * LENGTH, LENGTH), LENGTH)
        block = jnp.dot(pattern[index], values[rows, :], preferred_element_type=F32).astype(BF)
        for head in range(HEADS):
            mixed[rows, head * 128 : (head + 1) * 128] = block[head * LENGTH : (head + 1) * LENGTH]
        return carry

    counts[2] = count_z.finish()
    count_y.start()
    lax.fori_loop(0, 4, mix, 0)
    total_count = count_y.finish()[:, :1]
    loads["output"].wait()

    @pl.when(pipe == 1)
    def _():
        scale = jnp.full((1, 1), LIKELIHOOD_COEF * 128, F32) / total_count
        for pair in range(2):
            masks = [token_rows(pair, which) for which in range(2)]
            sums = [
                jnp.sum(masks[which][0] * logprob[pair, which : which + 1, :], axis=1, keepdims=True)
                for which in range(2)
            ]
            margin = DPO_BETA * (
                sums[0] - reference[pair, 0] - (sums[1] - reference[pair, 1])
            )
            pair_weight = jax.nn.sigmoid(-margin)
            chosen = -DPO_BETA * pair_weight * masks[0][1] - scale * masks[0][1]
            rejected = DPO_BETA * pair_weight * masks[1][1]
            mine = jnp.where(tensor == 0, chosen, rejected)
            theirs = jnp.where(tensor == 0, rejected, chosen)
            rows = pl.ds(pl.multiple_of((2 * pair + tensor) * LENGTH, LENGTH), LENGTH)
            upstream[rows, :] = (mine * head_own[pair].astype(F32)).astype(BF)
            if pair == 0:
                kept = theirs
        send_head.wait_send()
        send_weight.start()
        send_head.wait_recv()
        for pair, theirs in enumerate((kept, theirs)):
            rows = pl.ds(pl.multiple_of((2 * pair + 1 - tensor) * LENGTH, LENGTH), LENGTH)
            upstream[rows, :] = (theirs * head_other[pair].astype(F32)).astype(BF)

    @pl.when(pipe == 0)
    def _():
        pl.semaphore_wait(go, 1)
        send_weight.start()
        for send in send_below:
            send.wait_recv()

    def flow(size, place, ways, local, landing, hops):
        nonlocal base
        first = base
        made = Flow(
            size, place, *ways, local, lambda slot: landing.at[slot - first], sends, receives, base, hops
        )
        base += made.count
        return made

    z_halves = {(1, 0): 4, (-1, 1): 4, (1, 1): 3, (-1, 0): 3}
    y_halves = {(1, 0): 2, (-1, 1): 2, (1, 1): 1, (-1, 0): 1}
    z_whole = {(1, 0): 4, (-1, 0): 3}
    y_whole = {(1, 0): 2, (-1, 0): 1}
    rows_of = (pl.ds(0, 64), pl.ds(64, 48))
    a1 = flow(
        8, z, z_ways, lambda q, h: part_a.at[q, pl.ds(2 * h, 2), :, pl.ds(0, SPLIT)], land_a1, z_halves
    )
    v1 = flow(
        8,
        z,
        z_ways,
        lambda q, h: part_a.at[q, pl.ds(2 * h, 2), :, pl.ds(SPLIT, HEAD_DIM)],
        land_v1,
        z_halves,
    )
    b1 = flow(4, y, y_ways, lambda q, h: part_b.at[pl.ds(4 * h, 4), q], land_b1, y_halves)
    a2 = flow(4, y, y_ways, lambda q, h: part_a.at[z, q, rows_of[h]], land_a2, y_halves)
    b2 = flow(8, z, z_ways, lambda q, h: part_b.at[q, y, rows_of[h]], land_b2, z_halves)

    def shares(size, place, device_at, local, landing):
        nonlocal base
        made = Shares(size, place, device_at, local, landing, sends, receives, base)
        base += made.count
        return made

    g1 = shares(8, z, lambda at: device(at, y, x), part_g, land_g1)
    g2 = shares(4, y, lambda at: device(z, at, x), part_h, land_g2)

    def later_products(index, carry):
        at = pl.ds(pl.multiple_of(index * 896, 128), 896)
        places = pl.ds(2 * index, 2)
        turned = upstream[:, at].T
        upstream_turned[at, :] = turned
        block = jnp.dot(turned, mixed[:, SPLIT:], preferred_element_type=F32)
        part_b[places] = block.astype(BF).reshape(2, 4, 112, COLS)
        return carry

    def first_products(index, carry):
        at = pl.ds(pl.multiple_of(index * 896, 128), 896)
        places = pl.ds(2 * index, 2)
        block = jnp.dot(upstream_turned[at, :], mixed[:, :SPLIT], preferred_element_type=F32)
        part_a[places, :, :, :SPLIT] = block.astype(BF).reshape(2, 4, 112, SPLIT)
        return carry

    def value_products(index, carry):
        at = pl.ds(pl.multiple_of(index * 896, 128), 896)
        places = pl.ds(2 * index, 2)
        block = jnp.dot(normed[:, at].T, grad[...], preferred_element_type=F32)
        part_a[places, :, :, SPLIT:] = block.astype(BF).reshape(2, 4, 112, HEAD_DIM)
        return carry

    lax.fori_loop(0, 4, later_products, 0)
    b1.step(0)
    lax.fori_loop(0, 4, first_products, 0)
    a1.step(0)

    def heads_back(first, count):
        rows = pl.ds(pl.multiple_of(first * 128, 128), count * 128)
        block = lax.dot_general(
            upstream[...], weight_out[rows, :], (((1,), (1,)), ((), ())), preferred_element_type=F32
        ).astype(BF)
        for head in range(count):
            at = pl.ds(pl.multiple_of((first + head) * LENGTH, LENGTH), LENGTH)
            for index in range(4):
                mixed_grad[index, at, :] = block[
                    index * LENGTH : (index + 1) * LENGTH, head * 128 : (head + 1) * 128
                ]

    def two_heads(index, carry):
        heads_back(2 * index, 2)
        return carry

    lax.fori_loop(0, 3, two_heads, 0)
    heads_back(6, 1)

    def unmix(index, carry):
        rows = pl.ds(pl.multiple_of(index * LENGTH, LENGTH), LENGTH)
        grad[rows, :] = lax.dot_general(
            pattern[index], mixed_grad[index], (((0,), (0,)), ((), ())), preferred_element_type=F32
        ).astype(BF)
        return carry

    lax.fori_loop(0, 4, unmix, 0)
    send_grad.start()

    lax.fori_loop(0, 4, value_products, 0)
    v1.step(0)
    outputs = []
    for pair in range(2):
        own_rows = pl.ds(pl.multiple_of((2 * pair + tensor) * LENGTH, LENGTH), LENGTH)
        outputs.append(
            pltpu.make_async_copy(below.at[own_rows], cotangent_out.at[pair], load_sems.at[9 + pair])
        )

    def norm_back(index, total):
        at = pl.ds(pl.multiple_of(index * BLOCK, BLOCK), BLOCK)
        last_dims = (((1,), (1,)), ((), ()))
        mine = lax.dot_general(grad[...], weight[at, :], last_dims, preferred_element_type=F32)
        theirs = lax.dot_general(
            grad_other[...], weight_other[at, :], last_dims, preferred_element_type=F32
        )
        both = mine.astype(BF).astype(F32) + theirs.astype(BF).astype(F32)
        normed_grad[:, at] = both
        term = both * inputs[:, at].astype(F32)
        gain_row[:, at] = jnp.sum(term * wide(rms[...]), axis=0, keepdims=True)
        term = term * gain[:, at]
        return total + term[:, :128] + term[:, 128:]

    def norm_pass():
        send_grad.wait_recv()
        total = lax.fori_loop(0, BLOCKS, norm_back, jnp.zeros((TOKENS, 128), F32), unroll=2)
        mean = jnp.sum(total, axis=1, keepdims=True) / WIDTH
        slopes[...] = rms[...] * rms[...] * rms[...] * mean
        for place in range(32):
            part_g[place // 4, place % 4, :, :112] = gain_row[:, 112 * place : 112 * (place + 1)]
        g1.start()

    def below_pass(pair):
        rows = pl.ds(128 * pair, 128)

        def through(index, carry):
            at = pl.ds(pl.multiple_of(index * BLOCK, BLOCK), BLOCK)
            scaled = normed_grad[rows, at] * gain[:, at]
            slope = wide(slopes[rows, :])
            change = wide(rms[rows, :]) * scaled - inputs[rows, at].astype(F32) * slope
            below[rows, at] = (upstream[rows, at].astype(F32) + change).astype(BF)
            return carry

        lax.fori_loop(0, BLOCKS, through, 0)

    b1.step(1)
    a1.step(1)

    @pl.when(pipe == 1)
    def _():
        send_weight.wait_recv()
        pl.semaphore_signal(go, inc=1, device_id=partner, device_id_type=MESH)
        norm_pass()
        for pair in range(2):
            below_pass(pair)
            send_below[pair].start()
            outputs[pair].start()

    v1.step(1)

    @pl.when(pipe == 0)
    def _():
        send_weight.wait_recv()
        norm_pass()

    a1.step(2)
    b1.finish()
    b2.step(0)
    v1.step(2)
    a1.step(3)
    b2.step(1)
    v1.step(3)

    @pl.when(pipe == 0)
    def _():
        for pair in range(2):
            below_pass(pair)
            outputs[pair].start()

    b2.step(2)
    a1.finish()
    v1.finish()
    a2.step(0)
    part_h[...] = g1.finish()
    g2.start()
    b2.step(3)
    a2.step(1)
    b2.finish()

    def last(index, source, target):
        return pltpu.make_async_remote_copy(
            src_ref=source,
            dst_ref=target,
            send_sem=sends.at[base + index],
            recv_sem=receives.at[base + index],
            device_id=x_way,
            device_id_type=MESH,
        )

    finals = []

    def exchange(index, part):
        total = part[z, y].astype(F32)
        low, high = total[:56], total[56:]
        last_src[index] = jnp.where(x == 0, high, low).astype(BF)
        copy = last(index, last_src.at[index], landed_out.at[index])
        copy.start()
        finals.append(copy)
        kept[index] = jnp.where(x == 0, low, high)
        keep = pltpu.make_async_copy(kept.at[index], kept_out.at[index], load_sems.at[11 + index])
        keep.start()
        outputs.append(keep)

    exchange(1, part_b)
    gain_total = g2.finish()
    low, high = gain_total[:, :56], gain_total[:, 56:112]
    gain_last[:, :56] = jnp.where(x == 0, high, low)
    gain_copy = last(2, gain_last, gain_landed_out)
    gain_copy.start()
    finals.append(gain_copy)
    gain_kept[:, :56] = jnp.where(x == 0, low, high)
    gain_keep = pltpu.make_async_copy(gain_kept, gain_kept_out, load_sems.at[13])
    gain_keep.start()
    outputs.append(gain_keep)
    a2.finish()
    exchange(0, part_a)
    for copy in finals:
        copy.wait_recv()
    for made in (count_z, count_y, count_x, a1, v1, b1, a2, b2, g1, g2):
        made.drain()
    for copy in (*finals, send_weight, send_grad):
        copy.wait_send()
    for output in outputs:
        output.wait()

    @pl.when(pipe == 1)
    def _():
        for send in send_below:
            send.wait_send()


def last_kernel(
    kept_hbm,
    landed_hbm,
    gain_kept_hbm,
    gain_landed_hbm,
    cotangent_hbm,
    mixed_hbm,
    value_hbm,
    gain_hbm,
    cotangent_out,
    kept,
    landed,
    gain_kept,
    gain_landed,
    cotangent,
    mixed,
    value,
    gain,
    load_sems,
    store_sems,
):
    loads = [
        pltpu.make_async_copy(source, buffer, load_sems.at[index])
        for index, (source, buffer) in enumerate(
            (
                (kept_hbm, kept),
                (landed_hbm, landed),
                (gain_kept_hbm, gain_kept),
                (gain_landed_hbm, gain_landed),
                (cotangent_hbm, cotangent),
            )
        )
    ]
    stores = [
        pltpu.make_async_copy(buffer, target, store_sems.at[index])
        for index, (buffer, target) in enumerate(
            ((mixed, mixed_hbm), (value, value_hbm), (gain, gain_hbm), (cotangent, cotangent_out))
        )
    ]
    for load in loads:
        load.start()
    for load in loads[:4]:
        load.wait()
    total = kept[0] + landed[0].astype(F32)
    mixed[:, :SPLIT] = total[:, :SPLIT]
    value[...] = total[:, SPLIT:]
    mixed[:, SPLIT:] = kept[1] + landed[1].astype(F32)
    gain[...] = gain_kept[:, :56] + gain_landed[:, :56]
    for store in stores[:3]:
        store.start()
    loads[4].wait()
    stores[3].start()
    for store in stores:
        store.wait()


def written_out(arrays):
    hbm = pl.BlockSpec(memory_space=pl.ANY)
    shapes = (
        jax.ShapeDtypeStruct((56, HEADS * HEAD_DIM), F32),
        jax.ShapeDtypeStruct((56, HEAD_DIM), F32),
        jax.ShapeDtypeStruct((1, 56), F32),
        jax.ShapeDtypeStruct((2, LENGTH, WIDTH), BF),
    )
    return pl.pallas_call(
        last_kernel,
        out_shape=shapes,
        in_specs=[hbm] * 5,
        out_specs=(hbm,) * 4,
        scratch_shapes=[pltpu.VMEM(array.shape, array.dtype) for array in arrays]
        + [pltpu.VMEM(shape.shape, shape.dtype) for shape in shapes[:3]]
        + [pltpu.SemaphoreType.DMA((5,)), pltpu.SemaphoreType.DMA((4,))],
        compiler_params=pltpu.CompilerParams(vmem_limit_bytes=60_000_000),
    )(*arrays)


def body(
    hidden_in,
    attention_probs,
    norm_gain,
    value_weight,
    output_weight,
    head_grad,
    policy_logprob,
    reference_logprob,
    sequence_bounds,
):
    copies = 7 + 3 + 1 + 14 + 14 + 6 + 6 + 14 + 7 + 3 + 3
    hbm = pl.BlockSpec(memory_space=pl.ANY)
    results = pl.pallas_call(
        step_kernel,
        out_shape=(
            jax.ShapeDtypeStruct((2, 56, COLS), F32),
            jax.ShapeDtypeStruct((2, 56, COLS), BF),
            jax.ShapeDtypeStruct((1, 128), F32),
            jax.ShapeDtypeStruct((1, 128), F32),
            jax.ShapeDtypeStruct((2, LENGTH, WIDTH), BF),
        ),
        in_specs=[hbm] * 9,
        out_specs=(hbm,) * 5,
        scratch_shapes=[
            pltpu.SMEM((2, 3), jnp.int32),
            pltpu.SMEM((2, 2), F32),
            pltpu.VMEM((2, 2, LENGTH), F32),
            pltpu.VMEM((1, WIDTH), F32),
            pltpu.VMEM((TOKENS, WIDTH), BF),
            pltpu.VMEM((4, HEADS * LENGTH, LENGTH), BF),
            pltpu.VMEM((WIDTH, HEAD_DIM), BF),
            pltpu.VMEM((WIDTH, HEAD_DIM), BF),
            pltpu.VMEM((HEADS * HEAD_DIM, WIDTH), BF),
            pltpu.VMEM((2, LENGTH, WIDTH), BF),
            pltpu.VMEM((2, LENGTH, WIDTH), BF),
            pltpu.VMEM((TOKENS, WIDTH), BF),
            pltpu.VMEM((WIDTH, TOKENS), BF),
            pltpu.VMEM((TOKENS, WIDTH), BF),
            pltpu.VMEM((TOKENS, WIDTH), BF),
            pltpu.VMEM((TOKENS, HEAD_DIM), BF),
            pltpu.VMEM((TOKENS, HEADS * HEAD_DIM), BF),
            pltpu.VMEM((4, HEADS * LENGTH, HEAD_DIM), BF),
            pltpu.VMEM((TOKENS, HEAD_DIM), BF),
            pltpu.VMEM((TOKENS, HEAD_DIM), BF),
            pltpu.VMEM((TOKENS, WIDTH), F32),
            pltpu.VMEM((TOKENS, 128), F32),
            pltpu.VMEM((TOKENS, 128), F32),
            pltpu.VMEM((1, WIDTH), F32),
            pltpu.VMEM((3, 1, 128), F32),
            pltpu.VMEM((7, 1, 128), F32),
            pltpu.VMEM((3, 1, 128), F32),
            pltpu.VMEM((1, 1, 128), F32),
            pltpu.VMEM((8, 4, 112, COLS), BF),
            pltpu.VMEM((8, 4, 112, COLS), BF),
            pltpu.VMEM((8, 4, 1, 128), F32),
            pltpu.VMEM((4, 1, 128), F32),
            pltpu.VMEM((14, 2, 112, SPLIT), BF),
            pltpu.VMEM((14, 2, 112, HEAD_DIM), BF),
            pltpu.VMEM((6, 4, 112, COLS), BF),
            pltpu.VMEM((6, 64, COLS), BF),
            pltpu.VMEM((14, 64, COLS), BF),
            pltpu.VMEM((7, 4, 1, 128), F32),
            pltpu.VMEM((3, 1, 128), F32),
            pltpu.VMEM((2, 56, COLS), BF),
            pltpu.VMEM((2, 56, COLS), F32),
            pltpu.VMEM((1, 128), F32),
            pltpu.VMEM((1, 128), F32),
            pltpu.SemaphoreType.DMA((14,)),
            pltpu.SemaphoreType.DMA((5,)),
            pltpu.SemaphoreType.DMA((5,)),
            pltpu.SemaphoreType.REGULAR,
            pltpu.SemaphoreType.DMA((copies,)),
            pltpu.SemaphoreType.DMA((copies,)),
        ],
        compiler_params=pltpu.CompilerParams(
            collective_id=0, has_side_effects=True, vmem_limit_bytes=60_000_000
        ),
    )(
        sequence_bounds,
        reference_logprob,
        policy_logprob,
        norm_gain,
        hidden_in.reshape(TOKENS, WIDTH),
        attention_probs.reshape(4, HEADS * LENGTH, LENGTH),
        value_weight[0],
        output_weight[0],
        head_grad.reshape(2, LENGTH, WIDTH),
    )
    mixed_share, value_share, gain_share, own_output = written_out(results)
    return (
        own_output.reshape(1, 2, 1, LENGTH, WIDTH),
        value_share[None],
        mixed_share[None],
        gain_share,
    )


def solution(mesh):
    in_specs = (
        P("pipe", "dp", None, None, None),
        P("pipe", "dp", None, "tensor", None, None),
        P("pipe", None),
        P("pipe", None, "tensor"),
        P("pipe", "tensor", None),
        P("dp", "tensor", None, None),
        P("dp", None, None),
        P("dp", None),
        P("dp", None),
    )
    out_specs = (
        P("pipe", "dp", "tensor", None, None),
        P("pipe", "dp", "tensor"),
        P("pipe", "dp", "tensor"),
        P("pipe", "dp"),
    )
    return jax.shard_map(body, mesh=mesh, in_specs=in_specs, out_specs=out_specs, check_vma=False)
```

```python
import functools

import jax
import jax.numpy as jnp
from jax import lax
from jax.experimental import pallas as pl
from jax.experimental.pallas import tpu as pltpu
from jax.sharding import PartitionSpec as P

HEAD_DIM = 128
EPSILON = 1e-06
DPO_BETA = 0.25
LIKELIHOOD_COEF = 0.2
MESH = pl.DeviceIdType.MESH
BF = jnp.bfloat16
F32 = jnp.float32
COLS = 512
SPLIT = 384
CROSS = 128
NEAR = SPLIT - CROSS + HEAD_DIM


class Flow:
    def __init__(self, size, place, ahead, behind, local, landing, sends, receives, bases, hops):
        self.place, self.local, self.landing, self.hops = place, local, landing, hops
        self.target = {1: ahead, -1: behind}
        self.slot = {}
        for (way, half), count in hops.items():
            for step in range(count):
                self.slot[way, half, step] = len(self.slot)
        self.count = len(self.slot)
        self.halves = 1 + max(half for _, half in hops)
        self.copies, self.targets = {}, {}
        for (way, half, step), slot in self.slot.items():
            chunk = lax.rem(place + way * (hops[way, half] - step) + size, size)
            source = self.targets[way, half, step] = local(chunk, half)
            self.copies[way, half, step] = pltpu.make_async_remote_copy(
                src_ref=source,
                dst_ref=self.landed(slot, source),
                send_sem=sends.at[bases[0] + half],
                recv_sem=receives.at[bases[1] + slot],
                device_id=self.target[way],
                device_id_type=MESH,
            )
        self.drains = []
        for half in range(self.halves):
            sent = sum(count for (_, of), count in hops.items() if of == half)
            like = local(place, half)
            whole = landing.at[pl.ds(0, sent)]
            if landing.shape[1] != like.shape[0]:
                whole = landing.at[pl.ds(0, sent), pl.ds(0, like.shape[0])]
            self.drains.append(waiting(whole, sends.at[bases[0] + half], receives.at[bases[1]], ahead))

    def landed(self, slot, like):
        landing = self.landing.at[slot]
        if landing.shape == like.shape:
            return landing
        return landing.at[pl.ds(0, like.shape[0])]

    def collect(self, way, half, step, target):
        self.copies[way, half, step].wait_recv()
        add_into(target, self.landed(self.slot[way, half, step], target))

    def step(self, step):
        for way, half in self.hops:
            if step < self.hops[way, half]:
                if step:
                    self.collect(way, half, step - 1, self.targets[way, half, step])
                self.copies[way, half, step].start()

    def finish(self):
        for (way, half), count in self.hops.items():
            self.collect(way, half, count - 1, self.local(self.place, half))

    def drain(self):
        for copy in self.drains:
            copy.wait_send()


def waiting(whole, send_sem, recv_sem, device):
    return pltpu.make_async_remote_copy(
        src_ref=whole,
        dst_ref=whole,
        send_sem=send_sem,
        recv_sem=recv_sem,
        device_id=device,
        device_id_type=MESH,
    )


def add_into(target, landed):
    if len(target.shape) > 2 and target.shape[-2] > 1:

        def one(index, carry):
            target[index] = target[index] + landed[index]
            return carry

        lax.fori_loop(0, target.shape[0], one, 0)
    else:
        target[...] = target[...] + landed[...]


class Spread:
    def __init__(self, size, place, device_at, own, share_at, landing, sends, receives, bases):
        self.own, self.landing = own, landing
        send_sem, recv_sem = sends.at[bases[0]], receives.at[bases[1]]
        self.copies = []
        for slot in range(size - 1):
            at = lax.rem(place + 1 + slot, size)
            self.copies.append(
                pltpu.make_async_remote_copy(
                    src_ref=share_at(at),
                    dst_ref=landing.at[slot],
                    send_sem=send_sem,
                    recv_sem=recv_sem,
                    device_id=device_at(at),
                    device_id_type=MESH,
                )
            )
        self.all = waiting(landing, send_sem, recv_sem, device_at(lax.rem(place + 1, size)))

    def start(self):
        for copy in self.copies:
            copy.start()

    def finish(self):
        self.all.wait_recv()
        total = self.own[...]
        for slot in range(len(self.copies)):
            total = total + self.landing[slot]
        return total

    def drain(self):
        self.all.wait_send()


WIDTH = 3584
TOKENS = 256
BLOCK = 256
BLOCKS = WIDTH // BLOCK
LENGTH = 64
HEADS = 7


def wide(rows):
    return jnp.concatenate([rows, rows], axis=1)


def step_kernel(
    bounds_hbm,
    reference_hbm,
    logprob_hbm,
    gain_hbm,
    inputs_hbm,
    pattern_hbm,
    value_hbm,
    output_hbm,
    head_hbm,
    kept_out,
    landed_out,
    gain_kept_out,
    gain_landed_out,
    cotangent_out,
    bounds,
    reference,
    logprob,
    gain,
    inputs,
    pattern,
    weight,
    weight_other,
    weight_out,
    head_own,
    head_other,
    upstream,
    upstream_turned,
    below,
    normed,
    values,
    mixed,
    mixed_grad,
    grad,
    grad_other,
    normed_grad,
    rms,
    slopes,
    gain_row,
    counts,
    land_cz,
    land_cy,
    land_cx,
    part_a,
    part_b,
    part_c,
    part_g,
    part_h,
    land_a1,
    land_v1,
    land_b1,
    land_a2,
    land_b2,
    land_cross,
    land_c1,
    land_c2,
    land_g1,
    land_g2,
    last_src,
    kept,
    gain_last,
    gain_kept,
    load_sems,
    pass_sends,
    pass_receives,
    go,
    sends,
    receives,
):
    pipe = lax.axis_index("pipe")
    tensor = lax.axis_index("tensor")
    dp = lax.axis_index("dp")
    z = dp // 8
    y = lax.rem(dp, 8) // 2
    x = lax.rem(dp, 2)

    def device(z_at, y_at, x_at):
        return (pipe, z_at * 8 + y_at * 2 + x_at, tensor)

    z_next, z_prev = lax.rem(z + 1, 8), lax.rem(z + 7, 8)
    y_next, y_prev = lax.rem(y + 1, 4), lax.rem(y + 3, 4)
    z_ways = (device(z_next, y, x), device(z_prev, y, x))
    y_ways = (device(z, y_next, x), device(z, y_prev, x))
    x_way = device(z, y, 1 - x)
    peer = (pipe, dp, 1 - tensor)
    cross = (pipe, z * 8 + y * 2 + 1 - x, 1 - tensor)
    partner = (1 - pipe, dp, tensor)

    def token_rows(pair, which):
        lanes = lax.broadcasted_iota(jnp.int32, (1, LENGTH), 1)
        rows = lax.broadcasted_iota(jnp.int32, (LENGTH, 1), 0)
        first, end = bounds[pair, 0], bounds[pair, 1 + which]
        row_mask = ((lanes >= first) & (lanes < end)).astype(F32)
        column_mask = ((rows >= first) & (rows < end)).astype(F32)
        return row_mask, column_mask

    barrier = pltpu.get_barrier_semaphore()
    z_others = [device(lax.rem(z + step, 8), y, x) for step in range(1, 8)]
    y_others = [device(z, lax.rem(y + step, 4), x) for step in range(1, 4)]
    for neighbour in (*z_others, *y_others, x_way, peer, cross, partner):
        pl.semaphore_signal(barrier, inc=1, device_id=neighbour, device_id_type=MESH)
    loads = {
        name: pltpu.make_async_copy(source, target, load_sems.at[index])
        for index, (name, source, target) in enumerate(
            (
                ("head", head_hbm, head_own),
                ("bounds", bounds_hbm, bounds),
                ("reference", reference_hbm, reference),
                ("logprob", logprob_hbm, logprob),
                ("gain", gain_hbm, gain),
                ("inputs", inputs_hbm, inputs),
                ("weight", value_hbm, weight),
                ("pattern", pattern_hbm, pattern),
                ("output", output_hbm, weight_out),
            )
        )
    }
    for load in loads.values():
        load.start()

    for name in ("bounds", "reference", "logprob", "gain"):
        loads[name].wait()
    own_count = jnp.zeros((1, 1), F32)
    for pair in range(2):
        own_count = own_count + jnp.sum(token_rows(pair, 0)[0], axis=1, keepdims=True)
    counts[0] = jnp.broadcast_to(own_count, (1, 128))
    part_g[...] = jnp.zeros_like(part_g)
    gain_last[...] = jnp.zeros_like(gain_last)
    gain_kept[...] = jnp.zeros_like(gain_kept)
    pl.semaphore_wait(barrier, 14)
    loads["head"].wait()

    def passing(index, source, target, to):
        return pltpu.make_async_remote_copy(
            src_ref=source,
            dst_ref=target,
            send_sem=pass_sends.at[index],
            recv_sem=pass_receives.at[index],
            device_id=to,
            device_id_type=MESH,
        )

    send_head = passing(0, head_own, head_other, peer)
    send_weight = passing(1, weight, weight_other, cross)
    send_grad = passing(2, grad, grad_other, peer)
    send_below = [
        passing(3 + part, below.at[pl.ds(64 * part, 64)], upstream.at[pl.ds(64 * part, 64)], partner)
        for part in range(4)
    ]

    bases = (0, 0)

    def spread(size, place, device_at, own, share_at, landing):
        nonlocal bases
        made = Spread(size, place, device_at, own, share_at, landing, sends, receives, bases)
        bases = (bases[0] + 1, bases[1] + 1)
        return made

    def row_spread(size, place, device_at, own, landing):
        return spread(size, place, device_at, own, lambda at: own, landing)

    count_x = row_spread(2, x, lambda at: device(z, y, at), counts.at[0], land_cx)
    count_z = row_spread(8, z, lambda at: device(at, y, x), counts.at[1], land_cz)
    count_y = row_spread(4, y, lambda at: device(z, at, x), counts.at[2], land_cy)
    count_x.start()

    @pl.when(pipe == 1)
    def _():
        send_head.start()

    def flow(size, place, ways, local, landing, hops):
        nonlocal bases
        made = Flow(size, place, *ways, local, landing, sends, receives, bases, hops)
        bases = (bases[0] + made.halves, bases[1] + made.count)
        return made

    z_halves = {(1, 0): 4, (-1, 1): 4, (1, 1): 3, (-1, 0): 3}
    y_halves = {(1, 0): 2, (-1, 1): 2, (1, 1): 1, (-1, 0): 1}
    z_whole = {(1, 0): 4, (-1, 0): 3}
    y_whole = {(1, 0): 2, (-1, 0): 1}
    rows_of = (pl.ds(0, 64), pl.ds(64, 48))
    a1 = flow(
        8,
        z,
        z_ways,
        lambda q, h: part_a.at[q, pl.ds(2 * h, 2), :, pl.ds(0, NEAR - HEAD_DIM)],
        land_a1,
        z_halves,
    )
    v1 = flow(
        8,
        z,
        z_ways,
        lambda q, h: part_a.at[q, pl.ds(2 * h, 2), :, pl.ds(NEAR - HEAD_DIM, HEAD_DIM)],
        land_v1,
        z_halves,
    )
    cx = flow(2, x, (x_way, x_way), lambda q, h: part_c.at[q], land_cross, {(1, 0): 1})
    c1 = flow(8, z, z_ways, lambda q, h: part_c.at[x, q], land_c1, {(1, 0): 4, (-1, 0): 3})
    c2 = flow(4, y, y_ways, lambda q, h: part_c.at[x, z, q], land_c2, {(1, 0): 2, (-1, 0): 1})
    b1 = flow(4, y, y_ways, lambda q, h: part_b.at[pl.ds(4 * h, 4), q], land_b1, y_halves)
    a2 = flow(4, y, y_ways, lambda q, h: part_a.at[z, q, rows_of[h]], land_a2, y_halves)
    b2 = flow(8, z, z_ways, lambda q, h: part_b.at[q, y, rows_of[h]], land_b2, z_halves)

    g1 = spread(
        8, z, lambda at: device(at, y, x), part_g.at[z], lambda at: part_g.at[at], land_g1
    )
    g2 = spread(4, y, lambda at: device(z, at, x), part_h.at[y], lambda at: part_h.at[at], land_g2)

    loads["inputs"].wait()

    def square(index, total):
        at = pl.ds(pl.multiple_of(index * BLOCK, BLOCK), BLOCK)
        block = inputs[:, at].astype(F32)
        block = block * block
        return total + block[:, :128] + block[:, 128:]

    total = lax.fori_loop(0, BLOCKS, square, jnp.zeros((TOKENS, 128), F32))
    mean = jnp.sum(total, axis=1, keepdims=True) / WIDTH
    rms[...] = jnp.broadcast_to(lax.rsqrt(mean + EPSILON), (TOKENS, 128))
    counts[1] = count_x.finish()
    count_z.start()
    loads["weight"].wait()

    def project(index, total):
        at = pl.ds(pl.multiple_of(index * BLOCK, BLOCK), BLOCK)
        block = (inputs[:, at].astype(F32) * wide(rms[...]) * gain[:, at]).astype(BF)
        normed[:, at] = block
        return total + jnp.dot(block, weight[at, :], preferred_element_type=F32)

    total = lax.fori_loop(0, BLOCKS, project, jnp.zeros((TOKENS, 128), F32))
    values[...] = total.astype(BF)
    loads["pattern"].wait()

    def mix(index, carry):
        rows = pl.ds(pl.multiple_of(index * LENGTH, LENGTH), LENGTH)
        block = jnp.dot(pattern[index], values[rows, :], preferred_element_type=F32).astype(BF)
        for head in range(HEADS):
            mixed[rows, head * 128 : (head + 1) * 128] = block[head * LENGTH : (head + 1) * LENGTH]
        return carry

    counts[2] = count_z.finish()
    count_y.start()
    lax.fori_loop(0, 4, mix, 0)
    total_count = count_y.finish()[:, :1]
    loads["output"].wait()

    @pl.when(pipe == 1)
    def _():
        scale = jnp.full((1, 1), LIKELIHOOD_COEF * 128, F32) / total_count
        for pair in range(2):
            masks = [token_rows(pair, which) for which in range(2)]
            sums = [
                jnp.sum(masks[which][0] * logprob[pair, which : which + 1, :], axis=1, keepdims=True)
                for which in range(2)
            ]
            margin = DPO_BETA * (
                sums[0] - reference[pair, 0] - (sums[1] - reference[pair, 1])
            )
            pair_weight = jax.nn.sigmoid(-margin)
            chosen = -DPO_BETA * pair_weight * masks[0][1] - scale * masks[0][1]
            rejected = DPO_BETA * pair_weight * masks[1][1]
            mine = jnp.where(tensor == 0, chosen, rejected)
            theirs = jnp.where(tensor == 0, rejected, chosen)
            rows = pl.ds(pl.multiple_of((2 * pair + tensor) * LENGTH, LENGTH), LENGTH)
            upstream[rows, :] = (mine * head_own[pair].astype(F32)).astype(BF)
            if pair == 0:
                kept = theirs
        send_head.wait_send()
        send_weight.start()
        send_head.wait_recv()
        for pair, theirs in enumerate((kept, theirs)):
            rows = pl.ds(pl.multiple_of((2 * pair + 1 - tensor) * LENGTH, LENGTH), LENGTH)
            upstream[rows, :] = (theirs * head_other[pair].astype(F32)).astype(BF)

    @pl.when(pipe == 0)
    def _():
        pl.semaphore_wait(go, 1)
        send_weight.start()
        for send in send_below:
            send.wait_recv()

    def later_products(index, carry):
        at = pl.ds(pl.multiple_of(index * 896, 128), 896)
        places = pl.ds(2 * index, 2)
        turned = upstream[:, at].T
        upstream_turned[at, :] = turned
        block = jnp.dot(turned, mixed[:, SPLIT:], preferred_element_type=F32)
        part_b[places] = block.astype(BF).reshape(2, 4, 112, COLS)
        return carry

    def first_products(index, carry):
        at = pl.ds(pl.multiple_of(index * 896, 128), 896)
        places = pl.ds(2 * index, 2)
        block = jnp.dot(upstream_turned[at, :], mixed[:, :SPLIT], preferred_element_type=F32)
        crossing = block[:, :CROSS].reshape(2, 4, 2, 56, CROSS).astype(BF)
        for half in range(2):
            part_c[half, places] = crossing[:, :, half]
        part_a[places, :, :, : NEAR - HEAD_DIM] = (
            block[:, CROSS:].astype(BF).reshape(2, 4, 112, NEAR - HEAD_DIM)
        )
        return carry

    def value_products(index, carry):
        at = pl.ds(pl.multiple_of(index * 896, 128), 896)
        places = pl.ds(2 * index, 2)
        block = jnp.dot(normed[:, at].T, grad[...], preferred_element_type=F32)
        part_a[places, :, :, NEAR - HEAD_DIM :] = block.astype(BF).reshape(2, 4, 112, HEAD_DIM)
        return carry

    lax.fori_loop(0, 4, later_products, 0)
    b1.step(0)
    lax.fori_loop(0, 4, first_products, 0)
    @pl.when(pipe == 0)
    def _():
        cx.step(0)

    a1.step(0)

    def heads_back(first, count):
        rows = pl.ds(pl.multiple_of(first * 128, 128), count * 128)
        block = lax.dot_general(
            upstream[...], weight_out[rows, :], (((1,), (1,)), ((), ())), preferred_element_type=F32
        ).astype(BF)
        for head in range(count):
            at = pl.ds(pl.multiple_of((first + head) * LENGTH, LENGTH), LENGTH)
            for index in range(4):
                mixed_grad[index, at, :] = block[
                    index * LENGTH : (index + 1) * LENGTH, head * 128 : (head + 1) * 128
                ]

    def two_heads(index, carry):
        heads_back(2 * index, 2)
        return carry

    lax.fori_loop(0, 3, two_heads, 0)
    heads_back(6, 1)

    def unmix(index, carry):
        rows = pl.ds(pl.multiple_of(index * LENGTH, LENGTH), LENGTH)
        grad[rows, :] = lax.dot_general(
            pattern[index], mixed_grad[index], (((0,), (0,)), ((), ())), preferred_element_type=F32
        ).astype(BF)
        return carry

    lax.fori_loop(0, 4, unmix, 0)
    send_grad.start()

    @pl.when(pipe == 1)
    def _():
        cx.step(0)
        a1.step(1)

    lax.fori_loop(0, 4, value_products, 0)
    v1.step(0)

    def norm_back(index, total):
        at = pl.ds(pl.multiple_of(index * BLOCK, BLOCK), BLOCK)
        last_dims = (((1,), (1,)), ((), ()))
        mine = lax.dot_general(grad[...], weight[at, :], last_dims, preferred_element_type=F32)
        theirs = lax.dot_general(
            grad_other[...], weight_other[at, :], last_dims, preferred_element_type=F32
        )
        both = mine.astype(BF).astype(F32) + theirs.astype(BF).astype(F32)
        normed_grad[:, at] = both
        term = both * inputs[:, at].astype(F32)
        gain_row[:, at] = jnp.sum(term * wide(rms[...]), axis=0, keepdims=True)
        term = term * gain[:, at]
        return total + term[:, :128] + term[:, 128:]

    def norm_pass():
        send_grad.wait_recv()
        total = lax.fori_loop(0, BLOCKS, norm_back, jnp.zeros((TOKENS, 128), F32), unroll=2)
        mean = jnp.sum(total, axis=1, keepdims=True) / WIDTH
        slopes[...] = rms[...] * rms[...] * rms[...] * mean
        for place in range(32):
            part_g[place // 4, place % 4, :, :112] = gain_row[:, 112 * place : 112 * (place + 1)]
        g1.start()

    def below_pass(part):
        rows = pl.ds(LENGTH * part, LENGTH)

        def through(index, carry):
            at = pl.ds(pl.multiple_of(index * 512, 512), 512)
            scaled = normed_grad[rows, at] * gain[:, at]
            slope = wide(wide(slopes[rows, :]))
            change = wide(wide(rms[rows, :])) * scaled - inputs[rows, at].astype(F32) * slope
            below[rows, at] = (upstream[rows, at].astype(F32) + change).astype(BF)
            return carry

        lax.fori_loop(0, WIDTH // 512, through, 0)

    def write_below(passed=None):
        for part in range(4):
            below_pass(part)
            if passed:
                passed[part].start()
        copies = []
        for pair in range(2):
            own_rows = pl.ds(pl.multiple_of((2 * pair + tensor) * LENGTH, LENGTH), LENGTH)
            copy = pltpu.make_async_copy(
                below.at[own_rows], cotangent_out.at[pair], load_sems.at[9 + pair]
            )
            copy.start()
            copies.append(copy)
        return copies

    def last(index, source, target):
        return pltpu.make_async_remote_copy(
            src_ref=source,
            dst_ref=target,
            send_sem=sends.at[bases[0] + index],
            recv_sem=receives.at[bases[1] + index],
            device_id=x_way,
            device_id_type=MESH,
        )

    def keep(index, source, target):
        copy = pltpu.make_async_copy(source, target, load_sems.at[11 + index])
        copy.start()
        return copy

    def exchange(index, part, first):
        total = part[z, y].astype(F32)
        width = total.shape[1]
        at = pl.ds(first, width)
        low, high = total[:56], total[56:]
        last_src[:, at] = jnp.where(x == 0, high, low).astype(BF)
        copy = last(index, last_src.at[:, at], landed_out.at[:, at])
        copy.start()
        kept[:, at] = jnp.where(x == 0, low, high)
        return copy, keep(index, kept.at[:, at], kept_out.at[:, at])

    def keep_cross():
        at = pl.ds(NEAR + COLS, CROSS)
        kept[:, at] = part_c[x, z, y].astype(F32)
        return keep(2, kept.at[:, at], kept_out.at[:, at])

    def gain_middle():
        part_h[...] = g1.finish()
        g2.start()

    def gain_exchange():
        total = g2.finish()
        low, high = total[:, :56], total[:, 56:112]
        gain_last[:, :56] = jnp.where(x == 0, high, low)
        copy = last(2, gain_last, gain_landed_out)
        copy.start()
        gain_kept[:, :56] = jnp.where(x == 0, low, high)
        return copy, keep(3, gain_kept, gain_kept_out)

    def settle(finals, locals_):
        for copy in finals:
            copy.wait_recv()
        for made in (cx, a1, v1, b1, c1, a2, b2, c2, g1, g2):
            made.drain()
        for copy in finals:
            copy.wait_send()
        for copy in locals_:
            copy.wait()

    @pl.when(pipe == 1)
    def _():
        b1.step(1)
        send_weight.wait_recv()
        pl.semaphore_signal(go, inc=1, device_id=partner, device_id_type=MESH)
        norm_pass()
        a1.step(2)
        v1.step(1)
        copies = write_below(send_below)
        cx.finish()
        c1.step(0)
        a1.step(3)
        v1.step(2)
        b1.finish()
        b2.step(0)
        c1.step(1)
        a1.finish()
        v1.step(3)
        b2.step(1)
        c1.step(2)
        v1.finish()
        a2.step(0)
        b2.step(2)
        c1.step(3)
        gain_middle()
        a2.step(1)
        b2.step(3)
        c1.finish()
        c2.step(0)
        a2.finish()
        final_a, keep_a = exchange(0, part_a, 0)
        b2.finish()
        final_b, keep_b = exchange(1, part_b, NEAR)
        c2.step(1)
        final_g, keep_g = gain_exchange()
        c2.finish()
        keep_c = keep_cross()
        settle((final_a, final_b, final_g), (*copies, keep_a, keep_b, keep_g, keep_c))
        for send in send_below:
            send.wait_send()

    @pl.when(pipe == 0)
    def _():
        a1.step(1)
        b1.step(1)
        cx.finish()
        c1.step(0)
        v1.step(1)
        send_weight.wait_recv()
        norm_pass()
        a1.step(2)
        c1.step(1)
        v1.step(2)
        b1.finish()
        b2.step(0)
        a1.step(3)
        c1.step(2)
        v1.step(3)
        b2.step(1)
        a1.finish()
        c1.step(3)
        b2.step(2)
        v1.finish()
        a2.step(0)
        c1.finish()
        c2.step(0)
        gain_middle()
        b2.step(3)
        a2.step(1)
        c2.step(1)
        copies = write_below()
        b2.finish()
        final_b, keep_b = exchange(1, part_b, NEAR)
        a2.finish()
        final_a, keep_a = exchange(0, part_a, 0)
        final_g, keep_g = gain_exchange()
        c2.finish()
        keep_c = keep_cross()
        settle((final_a, final_b, final_g), (*copies, keep_a, keep_b, keep_g, keep_c))

    for made in (count_z, count_y, count_x):
        made.drain()
    for copy in (send_weight, send_grad):
        copy.wait_send()


def last_kernel(
    kept_hbm,
    landed_hbm,
    gain_kept_hbm,
    gain_landed_hbm,
    cotangent_hbm,
    mixed_hbm,
    value_hbm,
    gain_hbm,
    cotangent_out,
    kept,
    landed,
    gain_kept,
    gain_landed,
    cotangent,
    mixed,
    value,
    gain,
    load_sems,
    store_sems,
):
    loads = [
        pltpu.make_async_copy(source, buffer, load_sems.at[index])
        for index, (source, buffer) in enumerate(
            (
                (kept_hbm, kept),
                (landed_hbm, landed),
                (gain_kept_hbm, gain_kept),
                (gain_landed_hbm, gain_landed),
                (cotangent_hbm, cotangent),
            )
        )
    ]
    stores = [
        pltpu.make_async_copy(buffer, target, store_sems.at[index])
        for index, (buffer, target) in enumerate(
            ((mixed, mixed_hbm), (value, value_hbm), (gain, gain_hbm), (cotangent, cotangent_out))
        )
    ]
    for load in loads:
        load.start()
    for load in loads[:4]:
        load.wait()
    total = kept[:, : NEAR + COLS] + landed[...].astype(F32)
    mixed[:, :CROSS] = kept[:, NEAR + COLS :]
    mixed[:, CROSS:SPLIT] = total[:, : NEAR - HEAD_DIM]
    value[...] = total[:, NEAR - HEAD_DIM : NEAR]
    mixed[:, SPLIT:] = total[:, NEAR:]
    gain[...] = gain_kept[:, :56] + gain_landed[:, :56]
    for store in stores[:3]:
        store.start()
    loads[4].wait()
    stores[3].start()
    for store in stores:
        store.wait()


def written_out(arrays):
    hbm = pl.BlockSpec(memory_space=pl.ANY)
    shapes = (
        jax.ShapeDtypeStruct((56, HEADS * HEAD_DIM), F32),
        jax.ShapeDtypeStruct((56, HEAD_DIM), F32),
        jax.ShapeDtypeStruct((1, 56), F32),
        jax.ShapeDtypeStruct((2, LENGTH, WIDTH), BF),
    )
    return pl.pallas_call(
        last_kernel,
        out_shape=shapes,
        in_specs=[hbm] * 5,
        out_specs=(hbm,) * 4,
        scratch_shapes=[pltpu.VMEM(array.shape, array.dtype) for array in arrays]
        + [pltpu.VMEM(shape.shape, shape.dtype) for shape in shapes[:3]]
        + [pltpu.SemaphoreType.DMA((5,)), pltpu.SemaphoreType.DMA((4,))],
        compiler_params=pltpu.CompilerParams(vmem_limit_bytes=60_000_000),
    )(*arrays)


def body(
    hidden_in,
    attention_probs,
    norm_gain,
    value_weight,
    output_weight,
    head_grad,
    policy_logprob,
    reference_logprob,
    sequence_bounds,
):
    send_count, receive_count = 3 + 2 + 5 * 2 + 3 + 3, 3 + 2 + 14 + 14 + 6 + 6 + 14 + 1 + 7 + 3 + 3
    hbm = pl.BlockSpec(memory_space=pl.ANY)
    results = pl.pallas_call(
        step_kernel,
        out_shape=(
            jax.ShapeDtypeStruct((56, NEAR + COLS + CROSS), F32),
            jax.ShapeDtypeStruct((56, NEAR + COLS), BF),
            jax.ShapeDtypeStruct((1, 128), F32),
            jax.ShapeDtypeStruct((1, 128), F32),
            jax.ShapeDtypeStruct((2, LENGTH, WIDTH), BF),
        ),
        in_specs=[hbm] * 9,
        out_specs=(hbm,) * 5,
        scratch_shapes=[
            pltpu.SMEM((2, 3), jnp.int32),
            pltpu.SMEM((2, 2), F32),
            pltpu.VMEM((2, 2, LENGTH), F32),
            pltpu.VMEM((1, WIDTH), F32),
            pltpu.VMEM((TOKENS, WIDTH), BF),
            pltpu.VMEM((4, HEADS * LENGTH, LENGTH), BF),
            pltpu.VMEM((WIDTH, HEAD_DIM), BF),
            pltpu.VMEM((WIDTH, HEAD_DIM), BF),
            pltpu.VMEM((HEADS * HEAD_DIM, WIDTH), BF),
            pltpu.VMEM((2, LENGTH, WIDTH), BF),
            pltpu.VMEM((2, LENGTH, WIDTH), BF),
            pltpu.VMEM((TOKENS, WIDTH), BF),
            pltpu.VMEM((WIDTH, TOKENS), BF),
            pltpu.VMEM((TOKENS, WIDTH), BF),
            pltpu.VMEM((TOKENS, WIDTH), BF),
            pltpu.VMEM((TOKENS, HEAD_DIM), BF),
            pltpu.VMEM((TOKENS, HEADS * HEAD_DIM), BF),
            pltpu.VMEM((4, HEADS * LENGTH, HEAD_DIM), BF),
            pltpu.VMEM((TOKENS, HEAD_DIM), BF),
            pltpu.VMEM((TOKENS, HEAD_DIM), BF),
            pltpu.VMEM((TOKENS, WIDTH), F32),
            pltpu.VMEM((TOKENS, 128), F32),
            pltpu.VMEM((TOKENS, 128), F32),
            pltpu.VMEM((1, WIDTH), F32),
            pltpu.VMEM((3, 1, 128), F32),
            pltpu.VMEM((7, 1, 128), F32),
            pltpu.VMEM((3, 1, 128), F32),
            pltpu.VMEM((1, 1, 128), F32),
            pltpu.VMEM((8, 4, 112, NEAR), BF),
            pltpu.VMEM((8, 4, 112, COLS), BF),
            pltpu.VMEM((2, 8, 4, 56, CROSS), BF),
            pltpu.VMEM((8, 4, 1, 128), F32),
            pltpu.VMEM((4, 1, 128), F32),
            pltpu.VMEM((14, 2, 112, NEAR - HEAD_DIM), BF),
            pltpu.VMEM((14, 2, 112, HEAD_DIM), BF),
            pltpu.VMEM((6, 4, 112, COLS), BF),
            pltpu.VMEM((6, 64, NEAR), BF),
            pltpu.VMEM((14, 64, COLS), BF),
            pltpu.VMEM((1, 8, 4, 56, CROSS), BF),
            pltpu.VMEM((7, 4, 56, CROSS), BF),
            pltpu.VMEM((3, 56, CROSS), BF),
            pltpu.VMEM((7, 4, 1, 128), F32),
            pltpu.VMEM((3, 1, 128), F32),
            pltpu.VMEM((56, NEAR + COLS), BF),
            pltpu.VMEM((56, NEAR + COLS + CROSS), F32),
            pltpu.VMEM((1, 128), F32),
            pltpu.VMEM((1, 128), F32),
            pltpu.SemaphoreType.DMA((15,)),
            pltpu.SemaphoreType.DMA((7,)),
            pltpu.SemaphoreType.DMA((7,)),
            pltpu.SemaphoreType.REGULAR,
            pltpu.SemaphoreType.DMA((send_count,)),
            pltpu.SemaphoreType.DMA((receive_count,)),
        ],
        compiler_params=pltpu.CompilerParams(
            collective_id=0, has_side_effects=True, vmem_limit_bytes=60_000_000
        ),
    )(
        sequence_bounds,
        reference_logprob,
        policy_logprob,
        norm_gain,
        hidden_in.reshape(TOKENS, WIDTH),
        attention_probs.reshape(4, HEADS * LENGTH, LENGTH),
        value_weight[0],
        output_weight[0],
        head_grad.reshape(2, LENGTH, WIDTH),
    )
    mixed_share, value_share, gain_share, own_output = written_out(results)
    return (
        own_output.reshape(1, 2, 1, LENGTH, WIDTH),
        value_share[None],
        mixed_share[None],
        gain_share,
    )


def solution(mesh):
    in_specs = (
        P("pipe", "dp", None, None, None),
        P("pipe", "dp", None, "tensor", None, None),
        P("pipe", None),
        P("pipe", None, "tensor"),
        P("pipe", "tensor", None),
        P("dp", "tensor", None, None),
        P("dp", None, None),
        P("dp", None),
        P("dp", None),
    )
    out_specs = (
        P("pipe", "dp", "tensor", None, None),
        P("pipe", "dp", "tensor"),
        P("pipe", "dp", "tensor"),
        P("pipe", "dp"),
    )
    return jax.shard_map(body, mesh=mesh, in_specs=in_specs, out_specs=out_specs, check_vma=False)
```

```python
import functools

import jax
import jax.numpy as jnp
from jax import lax
from jax.experimental import pallas as pl
from jax.experimental.pallas import tpu as pltpu
from jax.sharding import PartitionSpec as P

HEAD_DIM = 128
EPSILON = 1e-06
DPO_BETA = 0.25
LIKELIHOOD_COEF = 0.2
MESH = pl.DeviceIdType.MESH
BF = jnp.bfloat16
F32 = jnp.float32
COLS = 512
SPLIT = 384
CROSS = 128
NEAR = SPLIT - CROSS + HEAD_DIM


class Flow:
    def __init__(self, size, place, ahead, behind, local, landing, sends, receives, bases, hops):
        self.place, self.local, self.landing, self.hops = place, local, landing, hops
        self.target = {1: ahead, -1: behind}
        self.slot = {}
        for (way, half), count in hops.items():
            for step in range(count):
                self.slot[way, half, step] = len(self.slot)
        self.count = len(self.slot)
        self.halves = 1 + max(half for _, half in hops)
        self.copies, self.targets = {}, {}
        for (way, half, step), slot in self.slot.items():
            chunk = lax.rem(place + way * (hops[way, half] - step) + size, size)
            source = self.targets[way, half, step] = local(chunk, half)
            self.copies[way, half, step] = pltpu.make_async_remote_copy(
                src_ref=source,
                dst_ref=self.landed(slot, source),
                send_sem=sends.at[bases[0] + half],
                recv_sem=receives.at[bases[1] + slot],
                device_id=self.target[way],
                device_id_type=MESH,
            )
        self.drains = []
        for half in range(self.halves):
            sent = sum(count for (_, of), count in hops.items() if of == half)
            like = local(place, half)
            whole = landing.at[pl.ds(0, sent)]
            if landing.shape[1] != like.shape[0]:
                whole = landing.at[pl.ds(0, sent), pl.ds(0, like.shape[0])]
            self.drains.append(waiting(whole, sends.at[bases[0] + half], receives.at[bases[1]], ahead))

    def landed(self, slot, like):
        landing = self.landing.at[slot]
        if landing.shape == like.shape:
            return landing
        return landing.at[pl.ds(0, like.shape[0])]

    def collect(self, way, half, step, target):
        self.copies[way, half, step].wait_recv()
        add_into(target, self.landed(self.slot[way, half, step], target))

    def step(self, step):
        for way, half in self.hops:
            if step < self.hops[way, half]:
                if step:
                    self.collect(way, half, step - 1, self.targets[way, half, step])
                self.copies[way, half, step].start()

    def finish(self):
        for (way, half), count in self.hops.items():
            self.collect(way, half, count - 1, self.local(self.place, half))

    def drain(self):
        for copy in self.drains:
            copy.wait_send()


def waiting(whole, send_sem, recv_sem, device):
    return pltpu.make_async_remote_copy(
        src_ref=whole,
        dst_ref=whole,
        send_sem=send_sem,
        recv_sem=recv_sem,
        device_id=device,
        device_id_type=MESH,
    )


def add_into(target, landed):
    if len(target.shape) > 2 and target.shape[-2] > 1:

        def one(index, carry):
            target[index] = target[index] + landed[index]
            return carry

        lax.fori_loop(0, target.shape[0], one, 0)
    else:
        target[...] = target[...] + landed[...]


class Spread:
    def __init__(self, size, place, device_at, own, share_at, landing, sends, receives, bases):
        self.own, self.landing = own, landing
        send_sem, recv_sem = sends.at[bases[0]], receives.at[bases[1]]
        self.copies = []
        for slot in range(size - 1):
            at = lax.rem(place + 1 + slot, size)
            self.copies.append(
                pltpu.make_async_remote_copy(
                    src_ref=share_at(at),
                    dst_ref=landing.at[slot],
                    send_sem=send_sem,
                    recv_sem=recv_sem,
                    device_id=device_at(at),
                    device_id_type=MESH,
                )
            )
        self.all = waiting(landing, send_sem, recv_sem, device_at(lax.rem(place + 1, size)))

    def start(self):
        for copy in self.copies:
            copy.start()

    def finish(self):
        self.all.wait_recv()
        total = self.own[...]
        for slot in range(len(self.copies)):
            total = total + self.landing[slot]
        return total

    def drain(self):
        self.all.wait_send()


WIDTH = 3584
TOKENS = 256
BLOCK = 256
BLOCKS = WIDTH // BLOCK
LENGTH = 64
HEADS = 7


def wide(rows):
    return jnp.concatenate([rows, rows], axis=1)


def step_kernel(
    bounds_hbm,
    reference_hbm,
    logprob_hbm,
    gain_hbm,
    inputs_hbm,
    pattern_hbm,
    value_hbm,
    output_hbm,
    head_hbm,
    kept_out,
    landed_out,
    gain_kept_out,
    gain_landed_out,
    cotangent_out,
    bounds,
    reference,
    logprob,
    gain,
    inputs,
    pattern,
    weight,
    weight_other,
    weight_out,
    head_own,
    head_other,
    upstream,
    upstream_turned,
    below,
    normed,
    values,
    mixed,
    mixed_grad,
    grad,
    grad_other,
    normed_grad,
    rms,
    slopes,
    gain_row,
    counts,
    land_cz,
    land_cy,
    land_cx,
    part_a,
    part_b,
    part_c,
    part_g,
    part_h,
    land_a1,
    land_v1,
    land_b1,
    land_a2,
    land_b2,
    land_cross,
    land_c1,
    land_c2,
    land_g1,
    land_g2,
    last_src,
    kept,
    gain_last,
    gain_kept,
    load_sems,
    pass_sends,
    pass_receives,
    go,
    sends,
    receives,
):
    pipe = lax.axis_index("pipe")
    tensor = lax.axis_index("tensor")
    dp = lax.axis_index("dp")
    z = dp // 8
    y = lax.rem(dp, 8) // 2
    x = lax.rem(dp, 2)

    def device(z_at, y_at, x_at):
        return (pipe, z_at * 8 + y_at * 2 + x_at, tensor)

    z_next, z_prev = lax.rem(z + 1, 8), lax.rem(z + 7, 8)
    y_next, y_prev = lax.rem(y + 1, 4), lax.rem(y + 3, 4)
    z_ways = (device(z_next, y, x), device(z_prev, y, x))
    y_ways = (device(z, y_next, x), device(z, y_prev, x))
    x_way = device(z, y, 1 - x)
    peer = (pipe, dp, 1 - tensor)
    cross = (pipe, z * 8 + y * 2 + 1 - x, 1 - tensor)
    partner = (1 - pipe, dp, tensor)

    def token_rows(pair, which):
        lanes = lax.broadcasted_iota(jnp.int32, (1, LENGTH), 1)
        rows = lax.broadcasted_iota(jnp.int32, (LENGTH, 1), 0)
        first, end = bounds[pair, 0], bounds[pair, 1 + which]
        row_mask = ((lanes >= first) & (lanes < end)).astype(F32)
        column_mask = ((rows >= first) & (rows < end)).astype(F32)
        return row_mask, column_mask

    barrier = pltpu.get_barrier_semaphore()
    z_others = [device(lax.rem(z + step, 8), y, x) for step in range(1, 8)]
    y_others = [device(z, lax.rem(y + step, 4), x) for step in range(1, 4)]
    for neighbour in (*z_others, *y_others, x_way, peer, cross, partner):
        pl.semaphore_signal(barrier, inc=1, device_id=neighbour, device_id_type=MESH)
    loads = {
        name: pltpu.make_async_copy(source, target, load_sems.at[index])
        for index, (name, source, target) in enumerate(
            (
                ("head", head_hbm, head_own),
                ("bounds", bounds_hbm, bounds),
                ("reference", reference_hbm, reference),
                ("logprob", logprob_hbm, logprob),
                ("gain", gain_hbm, gain),
                ("inputs", inputs_hbm, inputs),
                ("weight", value_hbm, weight),
                ("pattern", pattern_hbm, pattern),
                ("output", output_hbm, weight_out),
            )
        )
    }
    for load in loads.values():
        load.start()

    for name in ("bounds", "reference", "logprob", "gain"):
        loads[name].wait()
    own_count = jnp.zeros((1, 1), F32)
    for pair in range(2):
        own_count = own_count + jnp.sum(token_rows(pair, 0)[0], axis=1, keepdims=True)
    counts[0] = jnp.broadcast_to(own_count, (1, 128))
    part_g[...] = jnp.zeros_like(part_g)
    gain_last[...] = jnp.zeros_like(gain_last)
    gain_kept[...] = jnp.zeros_like(gain_kept)
    pl.semaphore_wait(barrier, 14)
    loads["head"].wait()

    def passing(index, source, target, to):
        return pltpu.make_async_remote_copy(
            src_ref=source,
            dst_ref=target,
            send_sem=pass_sends.at[index],
            recv_sem=pass_receives.at[index],
            device_id=to,
            device_id_type=MESH,
        )

    send_head = passing(0, head_own, head_other, peer)
    send_weight = passing(1, weight, weight_other, cross)
    send_grad = passing(2, grad, grad_other, peer)
    send_below = [
        passing(3 + part, below.at[pl.ds(64 * part, 64)], upstream.at[pl.ds(64 * part, 64)], partner)
        for part in range(4)
    ]

    bases = (0, 0)

    def spread(size, place, device_at, own, share_at, landing):
        nonlocal bases
        made = Spread(size, place, device_at, own, share_at, landing, sends, receives, bases)
        bases = (bases[0] + 1, bases[1] + 1)
        return made

    def row_spread(size, place, device_at, own, landing):
        return spread(size, place, device_at, own, lambda at: own, landing)

    count_x = row_spread(2, x, lambda at: device(z, y, at), counts.at[0], land_cx)
    count_z = row_spread(8, z, lambda at: device(at, y, x), counts.at[1], land_cz)
    count_y = row_spread(4, y, lambda at: device(z, at, x), counts.at[2], land_cy)
    count_x.start()

    @pl.when(pipe == 1)
    def _():
        send_head.start()

    def flow(size, place, ways, local, landing, hops):
        nonlocal bases
        made = Flow(size, place, *ways, local, landing, sends, receives, bases, hops)
        bases = (bases[0] + made.halves, bases[1] + made.count)
        return made

    z_halves = {(1, 0): 4, (-1, 1): 4, (1, 1): 3, (-1, 0): 3}
    y_halves = {(1, 0): 2, (-1, 1): 2, (1, 1): 1, (-1, 0): 1}
    z_whole = {(1, 0): 4, (-1, 0): 3}
    y_whole = {(1, 0): 2, (-1, 0): 1}
    rows_of = (pl.ds(0, 64), pl.ds(64, 48))
    a1 = flow(
        8,
        z,
        z_ways,
        lambda q, h: part_a.at[q, pl.ds(2 * h, 2), :, pl.ds(0, NEAR - HEAD_DIM)],
        land_a1,
        z_halves,
    )
    v1 = flow(
        8,
        z,
        z_ways,
        lambda q, h: part_a.at[q, pl.ds(2 * h, 2), :, pl.ds(NEAR - HEAD_DIM, HEAD_DIM)],
        land_v1,
        z_halves,
    )
    cx = flow(2, x, (x_way, x_way), lambda q, h: part_c.at[q], land_cross, {(1, 0): 1})
    c1 = flow(8, z, z_ways, lambda q, h: part_c.at[x, q], land_c1, {(1, 0): 4, (-1, 0): 3})
    c2 = flow(4, y, y_ways, lambda q, h: part_c.at[x, z, q], land_c2, {(1, 0): 2, (-1, 0): 1})
    b1 = flow(4, y, y_ways, lambda q, h: part_b.at[pl.ds(4 * h, 4), q], land_b1, y_halves)
    a2 = flow(4, y, y_ways, lambda q, h: part_a.at[z, q, rows_of[h]], land_a2, y_halves)
    b2 = flow(8, z, z_ways, lambda q, h: part_b.at[q, y, rows_of[h]], land_b2, z_halves)

    g1 = spread(
        8, z, lambda at: device(at, y, x), part_g.at[z], lambda at: part_g.at[at], land_g1
    )
    g2 = spread(4, y, lambda at: device(z, at, x), part_h.at[y], lambda at: part_h.at[at], land_g2)

    loads["inputs"].wait()

    def square(index, total):
        at = pl.ds(pl.multiple_of(index * BLOCK, BLOCK), BLOCK)
        block = inputs[:, at].astype(F32)
        block = block * block
        return total + block[:, :128] + block[:, 128:]

    total = lax.fori_loop(0, BLOCKS, square, jnp.zeros((TOKENS, 128), F32))
    mean = jnp.sum(total, axis=1, keepdims=True) / WIDTH
    rms[...] = jnp.broadcast_to(lax.rsqrt(mean + EPSILON), (TOKENS, 128))
    counts[1] = count_x.finish()
    count_z.start()
    loads["weight"].wait()

    def project(index, total):
        at = pl.ds(pl.multiple_of(index * BLOCK, BLOCK), BLOCK)
        block = (inputs[:, at].astype(F32) * wide(rms[...]) * gain[:, at]).astype(BF)
        normed[:, at] = block
        return total + jnp.dot(block, weight[at, :], preferred_element_type=F32)

    total = lax.fori_loop(0, BLOCKS, project, jnp.zeros((TOKENS, 128), F32))
    values[...] = total.astype(BF)
    loads["pattern"].wait()

    def mix(index, carry):
        rows = pl.ds(pl.multiple_of(index * LENGTH, LENGTH), LENGTH)
        block = jnp.dot(pattern[index], values[rows, :], preferred_element_type=F32).astype(BF)
        for head in range(HEADS):
            mixed[rows, head * 128 : (head + 1) * 128] = block[head * LENGTH : (head + 1) * LENGTH]
        return carry

    counts[2] = count_z.finish()
    count_y.start()
    lax.fori_loop(0, 4, mix, 0)
    total_count = count_y.finish()[:, :1]
    loads["output"].wait()

    @pl.when(pipe == 1)
    def _():
        scale = jnp.full((1, 1), LIKELIHOOD_COEF * 128, F32) / total_count
        for pair in range(2):
            masks = [token_rows(pair, which) for which in range(2)]
            sums = [
                jnp.sum(masks[which][0] * logprob[pair, which : which + 1, :], axis=1, keepdims=True)
                for which in range(2)
            ]
            margin = DPO_BETA * (
                sums[0] - reference[pair, 0] - (sums[1] - reference[pair, 1])
            )
            pair_weight = jax.nn.sigmoid(-margin)
            chosen = -DPO_BETA * pair_weight * masks[0][1] - scale * masks[0][1]
            rejected = DPO_BETA * pair_weight * masks[1][1]
            mine = jnp.where(tensor == 0, chosen, rejected)
            theirs = jnp.where(tensor == 0, rejected, chosen)
            rows = pl.ds(pl.multiple_of((2 * pair + tensor) * LENGTH, LENGTH), LENGTH)
            upstream[rows, :] = (mine * head_own[pair].astype(F32)).astype(BF)
            if pair == 0:
                kept = theirs
        send_head.wait_send()
        send_weight.start()
        send_head.wait_recv()
        for pair, theirs in enumerate((kept, theirs)):
            rows = pl.ds(pl.multiple_of((2 * pair + 1 - tensor) * LENGTH, LENGTH), LENGTH)
            upstream[rows, :] = (theirs * head_other[pair].astype(F32)).astype(BF)

    @pl.when(pipe == 0)
    def _():
        pl.semaphore_wait(go, 1)
        send_weight.start()
        for send in send_below:
            send.wait_recv()

    def later_products(index, carry):
        at = pl.ds(pl.multiple_of(index * 896, 128), 896)
        places = pl.ds(2 * index, 2)
        turned = upstream[:, at].T
        upstream_turned[at, :] = turned
        block = jnp.dot(turned, mixed[:, SPLIT:], preferred_element_type=F32)
        part_b[places] = block.astype(BF).reshape(2, 4, 112, COLS)
        return carry

    def first_products(index, carry):
        at = pl.ds(pl.multiple_of(index * 896, 128), 896)
        places = pl.ds(2 * index, 2)
        block = jnp.dot(upstream_turned[at, :], mixed[:, :SPLIT], preferred_element_type=F32)
        crossing = block[:, :CROSS].reshape(2, 4, 2, 56, CROSS).astype(BF)
        for half in range(2):
            part_c[half, places] = crossing[:, :, half]
        part_a[places, :, :, : NEAR - HEAD_DIM] = (
            block[:, CROSS:].astype(BF).reshape(2, 4, 112, NEAR - HEAD_DIM)
        )
        return carry

    def value_products(index, carry):
        at = pl.ds(pl.multiple_of(index * 896, 128), 896)
        places = pl.ds(2 * index, 2)
        block = jnp.dot(normed[:, at].T, grad[...], preferred_element_type=F32)
        part_a[places, :, :, NEAR - HEAD_DIM :] = block.astype(BF).reshape(2, 4, 112, HEAD_DIM)
        return carry

    lax.fori_loop(0, 4, later_products, 0)
    b1.step(0)
    lax.fori_loop(0, 4, first_products, 0)
    @pl.when(pipe == 0)
    def _():
        cx.step(0)

    a1.step(0)

    def heads_back(first, count):
        rows = pl.ds(pl.multiple_of(first * 128, 128), count * 128)
        block = lax.dot_general(
            upstream[...], weight_out[rows, :], (((1,), (1,)), ((), ())), preferred_element_type=F32
        ).astype(BF)
        for head in range(count):
            at = pl.ds(pl.multiple_of((first + head) * LENGTH, LENGTH), LENGTH)
            for index in range(4):
                mixed_grad[index, at, :] = block[
                    index * LENGTH : (index + 1) * LENGTH, head * 128 : (head + 1) * 128
                ]

    def two_heads(index, carry):
        heads_back(2 * index, 2)
        return carry

    lax.fori_loop(0, 3, two_heads, 0)
    heads_back(6, 1)

    def unmix(index, carry):
        rows = pl.ds(pl.multiple_of(index * LENGTH, LENGTH), LENGTH)
        grad[rows, :] = lax.dot_general(
            pattern[index], mixed_grad[index], (((0,), (0,)), ((), ())), preferred_element_type=F32
        ).astype(BF)
        return carry

    lax.fori_loop(0, 4, unmix, 0)
    send_grad.start()

    @pl.when(pipe == 1)
    def _():
        cx.step(0)
        a1.step(1)

    lax.fori_loop(0, 4, value_products, 0)
    v1.step(0)

    def norm_back(index, total):
        at = pl.ds(pl.multiple_of(index * BLOCK, BLOCK), BLOCK)
        last_dims = (((1,), (1,)), ((), ()))
        mine = lax.dot_general(grad[...], weight[at, :], last_dims, preferred_element_type=F32)
        theirs = lax.dot_general(
            grad_other[...], weight_other[at, :], last_dims, preferred_element_type=F32
        )
        both = mine.astype(BF).astype(F32) + theirs.astype(BF).astype(F32)
        normed_grad[:, at] = both
        term = both * inputs[:, at].astype(F32)
        gain_row[:, at] = jnp.sum(term * wide(rms[...]), axis=0, keepdims=True)
        term = term * gain[:, at]
        return total + term[:, :128] + term[:, 128:]

    def norm_pass():
        send_grad.wait_recv()
        total = lax.fori_loop(0, BLOCKS, norm_back, jnp.zeros((TOKENS, 128), F32), unroll=2)
        mean = jnp.sum(total, axis=1, keepdims=True) / WIDTH
        slopes[...] = rms[...] * rms[...] * rms[...] * mean
        for place in range(32):
            part_g[place // 4, place % 4, :, :112] = gain_row[:, 112 * place : 112 * (place + 1)]
        g1.start()

    def below_pass(part):
        rows = pl.ds(LENGTH * part, LENGTH)

        def through(index, carry):
            at = pl.ds(pl.multiple_of(index * 512, 512), 512)
            scaled = normed_grad[rows, at] * gain[:, at]
            slope = wide(wide(slopes[rows, :]))
            change = wide(wide(rms[rows, :])) * scaled - inputs[rows, at].astype(F32) * slope
            below[rows, at] = (upstream[rows, at].astype(F32) + change).astype(BF)
            return carry

        lax.fori_loop(0, WIDTH // 512, through, 0)

    def write_below(passed=None):
        for part in range(4):
            below_pass(part)
            if passed:
                passed[part].start()
        copies = []
        for pair in range(2):
            own_rows = pl.ds(pl.multiple_of((2 * pair + tensor) * LENGTH, LENGTH), LENGTH)
            copy = pltpu.make_async_copy(
                below.at[own_rows], cotangent_out.at[pair], load_sems.at[9 + pair]
            )
            copy.start()
            copies.append(copy)
        return copies

    def last(index, source, target):
        return pltpu.make_async_remote_copy(
            src_ref=source,
            dst_ref=target,
            send_sem=sends.at[bases[0] + index],
            recv_sem=receives.at[bases[1] + index],
            device_id=x_way,
            device_id_type=MESH,
        )

    def keep(index, source, target):
        copy = pltpu.make_async_copy(source, target, load_sems.at[11 + index])
        copy.start()
        return copy

    def exchange(index, part, first):
        total = part[z, y].astype(F32)
        width = total.shape[1]
        at = pl.ds(first, width)
        low, high = total[:56], total[56:]
        last_src[:, at] = jnp.where(x == 0, high, low).astype(BF)
        copy = last(index, last_src.at[:, at], landed_out.at[:, at])
        copy.start()
        kept[:, at] = jnp.where(x == 0, low, high)
        return copy, keep(index, kept.at[:, at], kept_out.at[:, at])

    def keep_cross():
        at = pl.ds(NEAR + COLS, CROSS)
        kept[:, at] = part_c[x, z, y].astype(F32)
        return keep(2, kept.at[:, at], kept_out.at[:, at])

    def gain_middle():
        part_h[...] = g1.finish()
        g2.start()

    def gain_exchange():
        total = g2.finish()
        low, high = total[:, :56], total[:, 56:112]
        gain_last[:, :56] = jnp.where(x == 0, high, low)
        copy = last(2, gain_last, gain_landed_out)
        copy.start()
        gain_kept[:, :56] = jnp.where(x == 0, low, high)
        return copy, keep(3, gain_kept, gain_kept_out)

    def settle(finals, locals_):
        for copy in finals:
            copy.wait_recv()
        for made in (cx, a1, v1, b1, c1, a2, b2, c2, g1, g2):
            made.drain()
        for copy in finals:
            copy.wait_send()
        for copy in locals_:
            copy.wait()

    @pl.when(pipe == 1)
    def _():
        b1.step(1)
        send_weight.wait_recv()
        pl.semaphore_signal(go, inc=1, device_id=partner, device_id_type=MESH)
        norm_pass()
        a1.step(2)
        v1.step(1)
        copies = write_below(send_below)
        cx.finish()
        c1.step(0)
        a1.step(3)
        v1.step(2)
        b1.finish()
        b2.step(0)
        c1.step(1)
        a1.finish()
        v1.step(3)
        b2.step(1)
        c1.step(2)
        v1.finish()
        a2.step(0)
        b2.step(2)
        c1.step(3)
        gain_middle()
        a2.step(1)
        b2.step(3)
        c1.finish()
        c2.step(0)
        a2.finish()
        final_a, keep_a = exchange(0, part_a, 0)
        b2.finish()
        final_b, keep_b = exchange(1, part_b, NEAR)
        c2.step(1)
        final_g, keep_g = gain_exchange()
        c2.finish()
        keep_c = keep_cross()
        settle((final_a, final_b, final_g), (*copies, keep_a, keep_b, keep_g, keep_c))
        for send in send_below:
            send.wait_send()

    @pl.when(pipe == 0)
    def _():
        a1.step(1)
        b1.step(1)
        cx.finish()
        c1.step(0)
        v1.step(1)
        send_weight.wait_recv()
        norm_pass()
        a1.step(2)
        c1.step(1)
        v1.step(2)
        b1.finish()
        b2.step(0)
        a1.step(3)
        copies = write_below()
        c1.step(2)
        b2.step(1)
        v1.step(3)
        a1.finish()
        c1.step(3)
        b2.step(2)
        v1.finish()
        a2.step(0)
        c1.finish()
        c2.step(0)
        gain_middle()
        b2.step(3)
        a2.step(1)
        c2.step(1)
        b2.finish()
        final_b, keep_b = exchange(1, part_b, NEAR)
        a2.finish()
        final_a, keep_a = exchange(0, part_a, 0)
        final_g, keep_g = gain_exchange()
        c2.finish()
        keep_c = keep_cross()
        settle((final_a, final_b, final_g), (*copies, keep_a, keep_b, keep_g, keep_c))

    for made in (count_z, count_y, count_x):
        made.drain()
    for copy in (send_weight, send_grad):
        copy.wait_send()


def last_kernel(
    kept_hbm,
    landed_hbm,
    gain_kept_hbm,
    gain_landed_hbm,
    cotangent_hbm,
    mixed_hbm,
    value_hbm,
    gain_hbm,
    cotangent_out,
    kept,
    landed,
    gain_kept,
    gain_landed,
    cotangent,
    mixed,
    value,
    gain,
    load_sems,
    store_sems,
):
    parts = [(pair, pl.ds(32 * half, 32)) for pair in range(2) for half in range(2)]
    loads = [
        pltpu.make_async_copy(source, buffer, load_sems.at[index])
        for index, (source, buffer) in enumerate(
            (
                (kept_hbm, kept),
                (landed_hbm, landed),
                (gain_kept_hbm, gain_kept),
                (gain_landed_hbm, gain_landed),
                *((cotangent_hbm.at[part], cotangent.at[part]) for part in parts),
            )
        )
    ]
    stores = [
        pltpu.make_async_copy(buffer, target, store_sems.at[index])
        for index, (buffer, target) in enumerate(
            (
                *((cotangent.at[part], cotangent_out.at[part]) for part in parts),
                (mixed, mixed_hbm),
                (value, value_hbm),
                (gain, gain_hbm),
            )
        )
    ]
    for load in loads:
        load.start()
    for load in loads[:4]:
        load.wait()
    total = kept[:, : NEAR + COLS] + landed[...].astype(F32)
    mixed[:, :CROSS] = kept[:, NEAR + COLS :]
    mixed[:, CROSS:SPLIT] = total[:, : NEAR - HEAD_DIM]
    value[...] = total[:, NEAR - HEAD_DIM : NEAR]
    mixed[:, SPLIT:] = total[:, NEAR:]
    gain[...] = gain_kept[:, :56] + gain_landed[:, :56]
    for store in stores[4:]:
        store.start()
    for load, store in zip(loads[4:], stores[:4]):
        load.wait()
        store.start()
    for store in stores:
        store.wait()


def written_out(arrays):
    hbm = pl.BlockSpec(memory_space=pl.ANY)
    shapes = (
        jax.ShapeDtypeStruct((56, HEADS * HEAD_DIM), F32),
        jax.ShapeDtypeStruct((56, HEAD_DIM), F32),
        jax.ShapeDtypeStruct((1, 56), F32),
        jax.ShapeDtypeStruct((2, LENGTH, WIDTH), BF),
    )
    return pl.pallas_call(
        last_kernel,
        out_shape=shapes,
        in_specs=[hbm] * 5,
        out_specs=(hbm,) * 4,
        scratch_shapes=[pltpu.VMEM(array.shape, array.dtype) for array in arrays]
        + [pltpu.VMEM(shape.shape, shape.dtype) for shape in shapes[:3]]
        + [pltpu.SemaphoreType.DMA((8,)), pltpu.SemaphoreType.DMA((7,))],
        compiler_params=pltpu.CompilerParams(vmem_limit_bytes=60_000_000),
    )(*arrays)


def body(
    hidden_in,
    attention_probs,
    norm_gain,
    value_weight,
    output_weight,
    head_grad,
    policy_logprob,
    reference_logprob,
    sequence_bounds,
):
    send_count, receive_count = 3 + 2 + 5 * 2 + 3 + 3, 3 + 2 + 14 + 14 + 6 + 6 + 14 + 1 + 7 + 3 + 3
    hbm = pl.BlockSpec(memory_space=pl.ANY)
    results = pl.pallas_call(
        step_kernel,
        out_shape=(
            jax.ShapeDtypeStruct((56, NEAR + COLS + CROSS), F32),
            jax.ShapeDtypeStruct((56, NEAR + COLS), BF),
            jax.ShapeDtypeStruct((1, 128), F32),
            jax.ShapeDtypeStruct((1, 128), F32),
            jax.ShapeDtypeStruct((2, LENGTH, WIDTH), BF),
        ),
        in_specs=[hbm] * 9,
        out_specs=(hbm,) * 5,
        scratch_shapes=[
            pltpu.SMEM((2, 3), jnp.int32),
            pltpu.SMEM((2, 2), F32),
            pltpu.VMEM((2, 2, LENGTH), F32),
            pltpu.VMEM((1, WIDTH), F32),
            pltpu.VMEM((TOKENS, WIDTH), BF),
            pltpu.VMEM((4, HEADS * LENGTH, LENGTH), BF),
            pltpu.VMEM((WIDTH, HEAD_DIM), BF),
            pltpu.VMEM((WIDTH, HEAD_DIM), BF),
            pltpu.VMEM((HEADS * HEAD_DIM, WIDTH), BF),
            pltpu.VMEM((2, LENGTH, WIDTH), BF),
            pltpu.VMEM((2, LENGTH, WIDTH), BF),
            pltpu.VMEM((TOKENS, WIDTH), BF),
            pltpu.VMEM((WIDTH, TOKENS), BF),
            pltpu.VMEM((TOKENS, WIDTH), BF),
            pltpu.VMEM((TOKENS, WIDTH), BF),
            pltpu.VMEM((TOKENS, HEAD_DIM), BF),
            pltpu.VMEM((TOKENS, HEADS * HEAD_DIM), BF),
            pltpu.VMEM((4, HEADS * LENGTH, HEAD_DIM), BF),
            pltpu.VMEM((TOKENS, HEAD_DIM), BF),
            pltpu.VMEM((TOKENS, HEAD_DIM), BF),
            pltpu.VMEM((TOKENS, WIDTH), F32),
            pltpu.VMEM((TOKENS, 128), F32),
            pltpu.VMEM((TOKENS, 128), F32),
            pltpu.VMEM((1, WIDTH), F32),
            pltpu.VMEM((3, 1, 128), F32),
            pltpu.VMEM((7, 1, 128), F32),
            pltpu.VMEM((3, 1, 128), F32),
            pltpu.VMEM((1, 1, 128), F32),
            pltpu.VMEM((8, 4, 112, NEAR), BF),
            pltpu.VMEM((8, 4, 112, COLS), BF),
            pltpu.VMEM((2, 8, 4, 56, CROSS), BF),
            pltpu.VMEM((8, 4, 1, 128), F32),
            pltpu.VMEM((4, 1, 128), F32),
            pltpu.VMEM((14, 2, 112, NEAR - HEAD_DIM), BF),
            pltpu.VMEM((14, 2, 112, HEAD_DIM), BF),
            pltpu.VMEM((6, 4, 112, COLS), BF),
            pltpu.VMEM((6, 64, NEAR), BF),
            pltpu.VMEM((14, 64, COLS), BF),
            pltpu.VMEM((1, 8, 4, 56, CROSS), BF),
            pltpu.VMEM((7, 4, 56, CROSS), BF),
            pltpu.VMEM((3, 56, CROSS), BF),
            pltpu.VMEM((7, 4, 1, 128), F32),
            pltpu.VMEM((3, 1, 128), F32),
            pltpu.VMEM((56, NEAR + COLS), BF),
            pltpu.VMEM((56, NEAR + COLS + CROSS), F32),
            pltpu.VMEM((1, 128), F32),
            pltpu.VMEM((1, 128), F32),
            pltpu.SemaphoreType.DMA((15,)),
            pltpu.SemaphoreType.DMA((7,)),
            pltpu.SemaphoreType.DMA((7,)),
            pltpu.SemaphoreType.REGULAR,
            pltpu.SemaphoreType.DMA((send_count,)),
            pltpu.SemaphoreType.DMA((receive_count,)),
        ],
        compiler_params=pltpu.CompilerParams(
            collective_id=0, has_side_effects=True, vmem_limit_bytes=60_000_000
        ),
    )(
        sequence_bounds,
        reference_logprob,
        policy_logprob,
        norm_gain,
        hidden_in.reshape(TOKENS, WIDTH),
        attention_probs.reshape(4, HEADS * LENGTH, LENGTH),
        value_weight[0],
        output_weight[0],
        head_grad.reshape(2, LENGTH, WIDTH),
    )
    mixed_share, value_share, gain_share, own_output = written_out(results)
    return (
        own_output.reshape(1, 2, 1, LENGTH, WIDTH),
        value_share[None],
        mixed_share[None],
        gain_share,
    )


def solution(mesh):
    in_specs = (
        P("pipe", "dp", None, None, None),
        P("pipe", "dp", None, "tensor", None, None),
        P("pipe", None),
        P("pipe", None, "tensor"),
        P("pipe", "tensor", None),
        P("dp", "tensor", None, None),
        P("dp", None, None),
        P("dp", None),
        P("dp", None),
    )
    out_specs = (
        P("pipe", "dp", "tensor", None, None),
        P("pipe", "dp", "tensor"),
        P("pipe", "dp", "tensor"),
        P("pipe", "dp"),
    )
    return jax.shard_map(body, mesh=mesh, in_specs=in_specs, out_specs=out_specs, check_vma=False)
```
